128 devices in a mesh: group: 32 (over x, z, core), tensor: 4 (over y).
Axes of the slice: x: 4, y: 4, z: 4, core: 2. Of those that a mesh axis runs over, the one named last changes fastest.
Arguments:
- queries: bfloat16 [4096, 4096], P('group', 'tensor'), may hold values from -120 to 120
- keys: bfloat16 [4096, 512], P('group', 'tensor'), may hold values from -6 to 6
- values: bfloat16 [4096, 512], P('group', 'tensor'), may hold values from -6 to 6
- document_index: int32 [32, 128], P('group'), may hold values from 0 to 7, never falling along the last dimension, each value on 1 to 64 neighbouring positions
- out_proj: bfloat16 [4096, 4096], P('tensor', 'group'), may hold values from -0.25 to 0.25
- residual_in: bfloat16 [4096, 4096], P(('group', 'tensor')), may hold values from -60 to 60
- norm_gain: float32 [4096], replicated, may hold values from 0.1 to 1.9
- expert_ids: int32 [4096, 8], P(('group', 'tensor')), may hold values from 0 to 127, all different within a row; in each aligned block of 32 rows (0 to 31, 32 to 63, ...) at most 4 rows name the same one
- gate_weights: float32 [4096, 8], P(('group', 'tensor')), may hold values from 0.05 to 0.45
- w_gate_up: bfloat16 [128, 4096, 1536], P(('group', 'tensor')), may hold values from -0.09375 to 0.09375
- w_down: bfloat16 [128, 768, 4096], P(('group', 'tensor')), may hold values from -0.21875 to 0.21875
Outputs:
- layer_out: bfloat16 [4096, 4096], P(('group', 'tensor'))
The draws below stay inside these ranges and needn't reach their ends.
Inputs may be any that keep to these rules, and one draw needn't show every extreme that they name: `document_index`: ids never fall along a group's tokens; equal ids mark one document. `expert_ids`: a token names 8 different experts; among the 32 tokens of one device (aligned blocks of rows) no expert is named more than 4 times, a bound that some block reaches.
All inputs are finite; a program needn't handle non-finite values.
Results may differ from the reference program's by a relative error of at most 0.0045.
Values may be sent and summed in bfloat16 or wider, within the bound.
A program may use at most 128 MiB of HBM per device.

```python
import math
import jax
import jax.numpy as jnp
import numpy as np
from jax import lax

D = 4096
QUERY_HEADS = 32
KEY_VALUE_HEADS = 4
HEAD_SIZE = 128
FF = 768
TOPK = 8
TOK_DEV = 32
GROUP_TOKENS = 128
TOTAL_TOKENS = 4096
EXPERTS = 128
CAP = 4
DOCS = 8
N_GROUP = 32


def draw_queries(key, part):
    final_output = jnp.clip(jax.random.normal(jax.random.fold_in(key, 1), (TOTAL_TOKENS, QUERY_HEADS * HEAD_SIZE), jnp.float32), -6.0, 6.0)
    return final_output.astype(jnp.bfloat16)


def draw_keys(key, part):
    final_output = jnp.clip(jax.random.normal(jax.random.fold_in(key, 2), (TOTAL_TOKENS, KEY_VALUE_HEADS * HEAD_SIZE), jnp.float32), -6.0, 6.0)
    return final_output.astype(jnp.bfloat16)


def draw_residual_in(key, part):
    row_scale = jnp.exp(jax.random.uniform(jax.random.fold_in(key, 11), (TOTAL_TOKENS, 1), jnp.float32, jnp.log(0.3), jnp.log(3.0)))
    column_scale = jnp.exp(jax.random.uniform(jax.random.fold_in(key, 12), (1, D), jnp.float32, jnp.log(0.3), jnp.log(3.0)))
    drawn_result = jnp.clip(jax.random.normal(jax.random.fold_in(key, 13), (TOTAL_TOKENS, D), jnp.float32), -6.0, 6.0)
    final_output = drawn_result * row_scale * column_scale
    return final_output.astype(jnp.bfloat16)


def block_scale(own_key, extent, split, low, largest):
    loudness = 1.0
    for dim, parts in split:
        draws = jax.random.uniform(jax.random.fold_in(jax.random.fold_in(own_key, 6), dim), (parts,), jnp.float32, low / len(split), largest / len(split))
        loudness = loudness * jnp.repeat(jnp.exp(draws), extent[dim] // parts).reshape((-1,) + (1,) * (len(extent) - 1 - dim))
    return loudness


def length_profile(number_of, total, limit, skew):
    portions = [(1 << 20) // math.isqrt(grade ** skew) + 1 for grade in range(2, number_of + 1)]
    surplus, given = total - limit - (number_of - 1), [1] * (number_of - 1)
    while surplus > 0:
        movable = [i for i in range(number_of - 1) if given[i] < limit]
        mass, remaining = sum([portions[i] for i in movable]), surplus
        for i in movable:
            more = min(limit - given[i], max(1, remaining * portions[i] // mass), surplus)
            given[i] = given[i] + more
            surplus = surplus - more
    return np.array([limit] + given)


def ragged_sizes(rng, number_of, total, bound, lean):
    if number_of == 2:
        one = jax.random.randint(rng, (), max(1, total - bound), min(bound, total - 1) + 1)
        return jnp.stack([one, total - one])
    sizes = jnp.asarray(length_profile(number_of, total, bound, lean), jnp.int32)
    couples = (number_of - 1) // 2
    donor, receiver = sizes[1:1 + 2 * couples:2], sizes[2:2 + 2 * couples:2]
    slack = jnp.minimum(donor - 1, bound - receiver)
    passed = jax.random.randint(jax.random.fold_in(rng, 1), (couples,), 0, 1 << 20) % (slack + 1)
    sizes = sizes.at[1:1 + 2 * couples:2].set(donor - passed).at[2:2 + 2 * couples:2].set(receiver + passed)
    return sizes[jax.random.permutation(jax.random.fold_in(rng, 2), number_of)]


def shared_out(own_key, own, number, rows, number_of, top, limit, slope):
    sequence = jax.random.permutation(own_key, number_of)
    packed, usual = shares(number_of, rows * top, limit, slope, True), shares(number_of, rows * top, limit, slope, False)
    places = jnp.arange(number_of)

    def named(tallies, offset_by):
        used = int((tallies > 0).sum())
        fixed = max(1, used // 4)
        passed = fixed + (places - fixed + offset_by * (used - fixed)) % max(1, number_of - fixed)
        return jnp.zeros((number_of,), jnp.int32).at[sequence[jnp.where(places < fixed, places, passed)]].set(jnp.asarray(tallies, jnp.int32))

    tallies = jnp.where(number % 4 == 0, named(packed, number // 4), named(usual, number - number // 4 - 1))
    mixed = jax.random.permutation(jax.random.fold_in(own, 3), number_of)
    donor, receiver = mixed[0:number_of // 2 * 2:2], mixed[1:number_of // 2 * 2:2]
    room = jnp.minimum(tallies[donor] - 1, limit - tallies[receiver]) // 2
    room = jnp.where((donor == sequence[0]) | (receiver == sequence[0]) | (tallies[receiver] == 0), 0, jnp.maximum(room, 0))
    passed = jax.random.randint(jax.random.fold_in(own, 4), (number_of // 2,), 0, 1 << 20) % (room + 1)
    tallies = tallies.at[donor].add(-passed).at[receiver].add(passed)
    items = jnp.searchsorted(jnp.cumsum(tallies), jnp.arange(rows * top), side="right").astype(jnp.int32)
    table = items.reshape(top, rows).T
    table = table[jax.random.permutation(jax.random.fold_in(own, 1), rows)]
    offset_by = jax.random.randint(jax.random.fold_in(own, 2), (rows, 1), 0, top)
    return jnp.take_along_axis(table, (jnp.arange(top)[None, :] + offset_by) % top, axis=1)


def shares(amount, total, limit, lean, full):
    portions = [(1 << 20) // math.isqrt(grade ** lean) + 1 for grade in range(1, amount + 1)]
    largest = limit if full else min(limit, max(-(-total // amount), total * portions[0] // sum(portions)))
    least = 1 if total - largest >= amount - 1 else 0
    counts, rest = [largest] + [least] * (amount - 1), total - largest - least * (amount - 1)
    while rest > 0:
        candidates = [i for i in range(1, amount) if counts[i] < largest] or [i for i in range(1, amount) if counts[i] < limit]
        whole, budget = sum([portions[i] for i in candidates]), rest
        for i in candidates:
            extra = min(limit - counts[i], max(1, budget * portions[i] // whole), rest)
            counts[i] = counts[i] + extra
            rest = rest - extra
    return np.array(counts)


def scatter_about(rng, shape, width, reach, shards=(), kind=jnp.bfloat16):
    entries = width * jax.random.normal(rng, shape, jnp.float32)
    if shards:
        entries = entries * block_scale(rng, shape, shards, -0.22, 0.18)
    return jnp.clip(entries, -reach, reach).astype(kind)


def setup_inputs(seed: int = 0) -> dict:
    streams_of = jax.random.split(jax.random.key(seed), 12)
    queries = draw_queries(jax.random.fold_in(streams_of[11], 71), 0)
    keys = draw_keys(jax.random.fold_in(streams_of[11], 71), 0)
    values = scatter_about(streams_of[2], (TOTAL_TOKENS, KEY_VALUE_HEADS * HEAD_SIZE), 1.0, 6.0, ((0, 32), (1, 4)))
    document_index = jax.vmap(lambda own: jnp.searchsorted(jnp.cumsum(ragged_sizes(own, DOCS, GROUP_TOKENS, GROUP_TOKENS // 2, 2)), jnp.arange(GROUP_TOKENS), side="right"))(jax.random.split(streams_of[3], N_GROUP)).reshape((N_GROUP, GROUP_TOKENS)).astype(jnp.int32)
    out_proj = scatter_about(streams_of[4], (QUERY_HEADS * HEAD_SIZE, D), (QUERY_HEADS * HEAD_SIZE // 8) ** -0.5, 0.25, ((0, 4), (1, 32)))
    residual_in = draw_residual_in(jax.random.fold_in(streams_of[11], 71), 0)
    norm_gain = jnp.clip(1.0 + 0.18 * jax.random.normal(streams_of[6], (D,), jnp.float32), 0.1, 1.9)
    expert_ids_keys = jax.random.split(jax.random.fold_in(streams_of[7], 1), TOTAL_TOKENS // TOK_DEV)
    expert_ids_turns = jax.random.permutation(jax.random.fold_in(streams_of[7], 3), TOTAL_TOKENS // TOK_DEV)
    expert_ids = jax.vmap(lambda own, number: shared_out(jax.random.fold_in(streams_of[7], 2), own, number, TOK_DEV, EXPERTS, TOPK, CAP, 2))(expert_ids_keys, expert_ids_turns).reshape((TOTAL_TOKENS, TOPK))
    gate_weights = jnp.clip(0.05 + 0.39999999 * jax.random.uniform(streams_of[8], (TOTAL_TOKENS, TOPK), jnp.float32) ** block_scale(streams_of[8], (TOTAL_TOKENS, TOPK), ((0, 128),), -0.2, 0.2), 0.05, 0.45)
    w_gate_up = scatter_about(streams_of[9], (EXPERTS, D, 2 * FF), D ** -0.5, 0.09375, ((0, 128),))
    w_down = scatter_about(streams_of[10], (EXPERTS, FF, D), FF ** -0.5, 0.21875, ((0, 128),))
    return dict(queries=queries, keys=keys, values=values, document_index=document_index, out_proj=out_proj, residual_in=residual_in, norm_gain=norm_gain, expert_ids=expert_ids, gate_weights=gate_weights, w_gate_up=w_gate_up, w_down=w_down)


def attend(query_matrix, key_matrix, value_matrix, doc_row):
    token_group = query_matrix.shape[0]
    query_head_split = query_matrix.reshape(token_group, KEY_VALUE_HEADS, QUERY_HEADS // KEY_VALUE_HEADS, HEAD_SIZE).astype(jnp.float32)
    key_head_split = key_matrix.reshape(token_group, KEY_VALUE_HEADS, HEAD_SIZE).astype(jnp.float32)
    value_head_split = value_matrix.reshape(token_group, KEY_VALUE_HEADS, HEAD_SIZE).astype(jnp.float32)
    scores = jnp.einsum('qgrd,kgd->grqk', query_head_split, key_head_split) * (1.0 / HEAD_SIZE ** 0.5)
    positions = jnp.arange(token_group, dtype=jnp.int32)
    visible = (positions[:, None] >= positions[None, :]) & (doc_row[:, None] == doc_row[None, :])
    scores = jnp.where(visible, scores, -jnp.inf)
    row_max = lax.optimization_barrier(jnp.max(scores, axis=-1, keepdims=True))
    exponent = jnp.where(visible, jnp.exp(scores - row_max), 0.0)
    weights = (exponent / lax.optimization_barrier(jnp.sum(exponent, axis=-1, keepdims=True))).astype(jnp.bfloat16)
    head_out = jnp.einsum('grqk,kgd->qgrd', weights.astype(jnp.float32), value_head_split)
    return head_out.astype(jnp.bfloat16).reshape(token_group, QUERY_HEADS * HEAD_SIZE)

def reference(queries, keys, values, document_index, out_proj, residual_in, norm_gain, expert_ids, gate_weights, w_gate_up, w_down):
    head_grouped = (queries.reshape(N_GROUP, GROUP_TOKENS, QUERY_HEADS * HEAD_SIZE), keys.reshape(N_GROUP, GROUP_TOKENS, KEY_VALUE_HEADS * HEAD_SIZE), values.reshape(N_GROUP, GROUP_TOKENS, KEY_VALUE_HEADS * HEAD_SIZE), document_index)

    def per_group(inputs):
        return attend(inputs[0], inputs[1], inputs[2], inputs[3])
    head_out = lax.map(per_group, head_grouped).reshape(TOTAL_TOKENS, QUERY_HEADS * HEAD_SIZE)
    hidden = residual_in.astype(jnp.float32) + jnp.dot(head_out, out_proj, preferred_element_type=jnp.float32)
    mean_square = lax.optimization_barrier(jnp.mean(hidden * hidden, axis=-1, keepdims=True))
    normed = (hidden * lax.rsqrt(mean_square + 1e-06) * norm_gain.astype(jnp.float32)).astype(jnp.bfloat16)
    flat_ids = expert_ids.reshape(-1).astype(jnp.int32)
    flat_gate = gate_weights.reshape(-1).astype(jnp.float32)
    token_index = (jnp.arange(TOTAL_TOKENS * TOPK, dtype=jnp.int32) // TOPK).astype(jnp.int32)
    slot_rows = EXPERTS * CAP

    def per_expert(moe_total, inputs):
        expert, gate_up, down_rows = inputs
        chosen = flat_ids == expert
        position = jnp.cumsum(chosen.astype(jnp.int32)) - 1
        position = jnp.where(chosen, position, slot_rows).astype(jnp.int32)
        sources = jnp.zeros((slot_rows,), jnp.int32).at[position].set(token_index, mode='drop')
        weight = jnp.zeros((slot_rows,), jnp.float32).at[position].set(flat_gate, mode='drop')
        gathered_rows = normed[sources]
        projected = jnp.dot(gathered_rows, gate_up, preferred_element_type=jnp.float32)
        activated = (jax.nn.silu(projected[:, :FF]) * projected[:, FF:]).astype(jnp.bfloat16)
        expert_out = jnp.dot(activated, down_rows, preferred_element_type=jnp.float32).astype(jnp.bfloat16)
        moe_total = moe_total.at[sources].add(expert_out.astype(jnp.float32) * weight[:, None])
        return (moe_total, None)
    moe_total, _ = lax.scan(per_expert, jnp.zeros((TOTAL_TOKENS, D), jnp.float32), (jnp.arange(EXPERTS, dtype=jnp.int32), w_gate_up, w_down))
    return (hidden + moe_total).astype(jnp.bfloat16)
```

```python
import functools

import jax
import jax.numpy as jnp
from jax import lax
from jax.experimental import pallas as pl
from jax.experimental.pallas import tpu as pltpu
from jax.sharding import PartitionSpec as P

HEAD = 128
MODEL = 4096
FF = 768
TOK = 32
CHUNKS = (
    (0, 0, 768, 0),
    (1, 1408, 640, 0),
    (2, 2688, 640, 0),
    (0, 768, 640, 1),
    (1, 2048, 640, 1),
    (2, 3328, 768, 1),
)
BF = jnp.bfloat16
F32 = jnp.float32


def dot(a, b):
    return jnp.dot(a, b, preferred_element_type=F32)


def device(x, y, z, c):
    return {"group": (x * 4 + z) * 2 + c, "tensor": y}


def plane_index(a, x, y, z, c):
    if a == 0:
        return c * 16 + z * 4 + y
    if a == 1:
        return c * 16 + z * 4 + x
    return c * 16 + x * 4 + y


def plane_partner(a, x, y, z, c, k):
    nc = lax.rem(c + lax.rem(k, 2), 2)
    lo = lax.rem(k // 2, 4)
    hi = k // 8
    if a == 0:
        return x, lax.rem(y + lo, 4), lax.rem(z + hi, 4), nc
    if a == 1:
        return lax.rem(x + lo, 4), y, lax.rem(z + hi, 4), nc
    return lax.rem(x + hi, 4), lax.rem(y + lo, 4), z, nc


def line_partner(a, x, y, z, d):
    if a == 0:
        return lax.rem(x + d, 4), y, z
    if a == 1:
        return x, lax.rem(y + d, 4), z
    return x, y, lax.rem(z + d, 4)


def axis_row(a, canon):
    r = canon & 3
    y = (canon >> 2) & 3
    x = (canon >> 4) & 3
    z = (canon >> 6) & 3
    if a == 0:
        return z * 64 + y * 16 + x * 4 + r
    return x * 64 + y * 16 + z * 4 + r


def iota(shape, dim):
    return lax.broadcasted_iota(jnp.int32, shape, dim)


def kernel(
    q_ref, k_ref, v_ref, doc_ref, wo_ref, res_ref, gain_ref, meta_ref, w1_hbm, w2_hbm, out_ref, *scratch
):
    n = len(CHUNKS)
    (w1, w2, b_buf, a_buf, c_send, c_recv, hid, proj, act, act_p, meta_all, sel, wgt_hi, wgt_lo, perm, perm_t) = scratch[:16]
    rest = scratch[16:]
    gath, slot_send, slot_recv, ret_recv, part, part_recv = (rest[i * n : (i + 1) * n] for i in range(6))
    (
        w_sem, b_send_sem, b_recv_sem, b_sib_sem, a_send_sem, a_recv_sem, c_send_sem, c_recv_sem, m_send_sem, m_recv_sem,
        g_send_sem, g_recv_sem, s_send_sem, s_recv_sem, y_send_sem, y_recv_sem, z_send_sem, z_recv_sem,
    ) = rest[6 * n :]

    g = lax.axis_index("group")
    y = lax.axis_index("tensor")
    x = g // 8
    z = lax.rem(g // 2, 4)
    c = lax.rem(g, 2)
    me = (x, y, z, c)
    along = (x, y, z)

    def remote(src, dst, send, recv, to):
        return pltpu.make_async_remote_copy(
            src_ref=src, dst_ref=dst, send_sem=send, recv_sem=recv, device_id=device(*to)
        )

    def wait_bytes(ref, sem):
        pltpu.make_async_copy(ref, ref, sem).wait()

    barrier = pltpu.get_barrier_semaphore()

    def greet(i, _):
        pl.semaphore_signal(
            barrier,
            inc=1,
            device_id={"group": lax.rem(g + i // 4, 32), "tensor": lax.rem(y + lax.rem(i, 4), 4)},
        )
        return 0

    lax.fori_loop(1, 128, greet, 0)

    loads = []
    for i in range(4):
        loads.append(
            pltpu.make_async_copy(w1_hbm.at[0, pl.ds(i * 1024, 1024)], w1.at[pl.ds(i * 1024, 1024)], w_sem.at[i])
        )
    for i in range(2):
        loads.append(
            pltpu.make_async_copy(w2_hbm.at[0, pl.ds(i * 384, 384)], w2.at[pl.ds(i * 384, 384)], w_sem.at[4 + i])
        )
    for copy in loads:
        copy.start()

    doc = jnp.broadcast_to(doc_ref[...].astype(F32), (128, 128))
    visible = (doc == doc.T) & (iota((128, 128), 0) >= iota((128, 128), 1))
    keys = k_ref[...]
    vals = v_ref[...]

    def attend(h):
        query = q_ref[:, h * HEAD : (h + 1) * HEAD]
        scores = lax.dot_general(query, keys, (((1,), (1,)), ((), ())), preferred_element_type=F32)
        scores = jnp.where(visible, scores * (1.0 / HEAD**0.5), -1e30)
        top = jnp.max(scores, axis=-1, keepdims=True)
        expo = jnp.where(visible, jnp.exp(scores - top), 0.0)
        weights = (expo / jnp.sum(expo, axis=-1, keepdims=True)).astype(BF)
        a_buf[z, :, h * HEAD : (h + 1) * HEAD] = dot(weights, vals).astype(BF)

    def send_heads(half):
        cols = pl.ds(half * 512, 512)
        for d in (1, 3, 2):
            to = (x, y, lax.rem(z + d, 4), c)
            remote(a_buf.at[z, :, cols], a_buf.at[z, :, cols], a_send_sem, a_recv_sem.at[d - 1], to).start()

    def b_cols(xx, cc):
        return pl.ds(pl.multiple_of((xx * 2 + cc) * 128, 128), 128)

    for h in range(4):
        attend(h)
    pl.semaphore_wait(barrier, 127)
    sibling = (x, y, z, 1 - c)
    for d in (2, 1, 3):
        to = (lax.rem(x + d, 4), y, z, c)
        remote(wo_ref, b_buf.at[:, b_cols(x, c)], b_send_sem, b_recv_sem.at[d - 1], to).start()
    remote(wo_ref, b_buf.at[:, b_cols(x, c)], b_send_sem, b_sib_sem, sibling).start()
    send_heads(0)
    for a in range(3):
        for d in (1, 3, 2):
            to = line_partner(a, x, y, z, d) + (c,)
            remote(meta_ref, meta_all.at[a, along[a]], m_send_sem, m_recv_sem, to).start()
    for h in range(4, 8):
        attend(h)
    send_heads(1)
    b_buf[:, b_cols(x, c)] = wo_ref[...]

    for a in range(3):
        meta_all[a, along[a]] = meta_ref[...]
    canon = iota((256, 256), 0)
    canon_t = iota((256, 256), 1)
    for i, a in enumerate((0, 2)):
        perm[i] = (iota((256, 256), 1) == axis_row(a, canon)).astype(F32).astype(BF)
        perm_t[i] = (iota((256, 256), 0) == axis_row(a, canon_t)).astype(F32).astype(BF)
    wait_bytes(meta_all9(meta_all), m_recv_sem)
    lane = iota((128, 128), 1)
    row = iota((128, 128), 0)
    earlier = (((row >> 5) == (lane >> 5)) & (row < lane)).astype(F32).astype(BF)
    slot = iota((512, 128), 0)
    slot_lane = iota((512, 128), 1)
    for a in range(3):
        meta = jnp.zeros((16, 128), F32)
        for s in range(4):
            meta = jnp.where((iota((16, 128), 1) >> 5) == s, meta_all[a, s], meta)
        named = jnp.zeros((128, 128), F32)
        gate = jnp.zeros((128, 128), F32)
        row_f = row.astype(F32)
        for k in range(8):
            hit = jnp.broadcast_to(meta[k : k + 1], (128, 128)) == row_f
            named = jnp.where(hit, 1.0, named)
            gate = jnp.where(hit, jnp.broadcast_to(meta[8 + k : 9 + k], (128, 128)), gate)
        place = dot(named.astype(BF), earlier)
        place = jnp.where(named > 0.5, place + 1.0, 0.0).astype(BF)
        gate_hi = gate.astype(BF)
        gate_lo = (gate - gate_hi.astype(F32)).astype(BF)
        j = slot >> 4
        jc, jh, jl = j >> 4, (j >> 2) & 3, j & 3
        if a == 0:
            ex, ey, ez = x, jl, jh
        elif a == 1:
            ex, ey, ez = jl, y, jh
        else:
            ex, ey, ez = jh, jl, z
        expert = ((ex * 4 + ez) * 2 + jc) * 4 + ey
        pick = (slot_lane == expert).astype(F32).astype(BF)
        match = (dot(pick, place) == ((slot & 3) + 1).astype(F32)) & ((slot_lane >> 5) == ((slot >> 2) & 3))
        sel[a] = jnp.where(match, 1.0, 0.0).astype(BF)
        wgt_hi[a] = jnp.where(match, dot(pick, gate_hi), 0.0).T.astype(BF)
        wgt_lo[a] = jnp.where(match, dot(pick, gate_lo), 0.0).T.astype(BF)

    for d in (1, 3, 2):
        src = lax.rem(x + 4 - d, 4)
        block = b_buf.at[:, b_cols(src, c)]
        wait_bytes(block, b_recv_sem.at[d - 1])
        remote(block, block, b_send_sem, b_sib_sem, sibling).start()
    wait_bytes(b_buf.at[:, pl.ds(0, 512)], b_sib_sem)
    for d in (0, 1, 3, 2):
        zz = lax.rem(z + 4 - d, 4)
        if d:
            wait_bytes(a_buf.at[zz], a_recv_sem.at[d - 1])

        def project(t, _, zz=zz):
            cols = pl.ds(pl.multiple_of(t * 256, 256), 256)
            c_send[zz, :, cols] = dot(a_buf[zz], b_buf[:, cols]).astype(BF)
            return 0

        lax.fori_loop(0, 4, project, 0)
        for dy in (1, 3, 2, 0):
            yy = lax.rem(y + dy, 4)
            rows = pl.ds(pl.multiple_of(yy * TOK, TOK), TOK)
            if d or dy:
                remote(
                    c_send.at[zz, rows, :], c_recv.at[y * 4 + z], c_send_sem, c_recv_sem, (x, yy, zz, c)
                ).start()
            else:
                c_recv[y * 4 + z] = c_send[zz, rows, :]
    wait_bytes(c_recv.at[pl.ds(0, 15)], c_recv_sem)
    square = jnp.zeros((TOK, 256), F32)
    for zz in range(4):
        for xx in range(4):
            col = (xx * 4 + zz) * 256
            value = res_ref[:, col : col + 256].astype(F32)
            for yy in range(4):
                value = value + c_recv[yy * 4 + zz, :, xx * 256 : (xx + 1) * 256].astype(F32)
            hid[:, col : col + 256] = value
            square = square + value * value
    scale = lax.rsqrt(jnp.sum(square, axis=-1, keepdims=True) * (1.0 / MODEL) + 1e-06)

    for i, (a, col, width, _) in enumerate(CHUNKS):
        normed = (hid[:, col : col + width] * scale * gain_ref[:, col : col + width]).astype(BF)
        gath[i][along[a]] = normed
        for d in (1, 3, 2):
            to = line_partner(a, x, y, z, d) + (c,)
            mine = gath[i].at[along[a]]
            remote(mine, mine, g_send_sem.at[i], g_recv_sem.at[i], to).start()

    def exchange(group, sources, targets, send_sem, recv_sem):
        members = [i for i in range(n) if CHUNKS[i][3] == group]

        def step(k, _):
            for i in members:
                a = CHUNKS[i][0]
                to = plane_partner(a, *me, k)
                remote(
                    sources[i].at[plane_index(a, *to)],
                    targets[i].at[plane_index(a, *me)],
                    send_sem.at[i],
                    recv_sem.at[i],
                    to,
                ).start()
            return 0

        lax.fori_loop(1, 32, step, 0)
        for i in members:
            mine = plane_index(CHUNKS[i][0], *me)
            targets[i][mine] = sources[i][mine]

    for group in range(2):
        for i, (a, col, width, grp) in enumerate(CHUNKS):
            if grp == group:
                wait_bytes(gath[i].at[pl.ds(0, 3)], g_recv_sem.at[i])
                rows = dot(sel[a], gath[i][...].reshape(128, width))
                slot_send[i][...] = rows.astype(BF).reshape(32, 16, width)
        exchange(group, slot_send, slot_recv, s_send_sem, s_recv_sem)

    for copy in loads:
        copy.wait()

    for group in range(2):
        members = [i for i in range(n) if CHUNKS[i][3] == group]
        for i in members:
            a, col, width, _ = CHUNKS[i]
            wait_bytes(slot_recv[i].at[pl.ds(0, 31)], s_recv_sem.at[i])
            if a != 1:
                for half in range(2):
                    block = slot_recv[i][half * 16 : half * 16 + 16].reshape(256, width)
                    moved = dot(perm[a // 2], block).astype(BF)
                    slot_recv[i][half * 16 : half * 16 + 16] = moved.reshape(16, 16, width)

        def up(t, _, members=members, group=group):
            cols = pl.ds(pl.multiple_of(t * 256, 256), 256)
            total = proj[:, cols] if group else jnp.zeros((512, 256), F32)
            for i in members:
                _, col, width, _ = CHUNKS[i]
                total = total + dot(slot_recv[i][...].reshape(512, width), w1[col : col + width, cols])
            proj[:, cols] = total
            return 0

        lax.fori_loop(0, 6, up, 0)

    def activate(t, _):
        rows = pl.ds(pl.multiple_of(t * 64, 64), 64)
        gate = proj[rows, :FF]
        act[rows, :] = (gate / (1.0 + jnp.exp(-gate)) * proj[rows, FF:]).astype(BF)
        return 0

    lax.fori_loop(0, 8, activate, 0)
    for i in range(2):
        for half in range(2):
            rows = slice(half * 256, half * 256 + 256)
            act_p[i, rows, :] = dot(perm_t[i], act[rows, :]).astype(BF)

    for group in range(2):
        for i, (a, col, width, grp) in enumerate(CHUNKS):
            if grp == group:
                wait_bytes(slot_send[i].at[pl.ds(0, 31)], s_send_sem.at[i])
                for t in range(0, width, 128):
                    mine = act[...] if a == 1 else act_p[a // 2]
                    rows = dot(mine, w2[:, col + t : col + t + 128]).astype(BF)
                    slot_send[i][:, :, t : t + 128] = rows.reshape(32, 16, 128)
        exchange(group, slot_send, ret_recv, y_send_sem, y_recv_sem)

    for group in range(2):
        for i, (a, col, width, grp) in enumerate(CHUNKS):
            if grp == group:
                wait_bytes(ret_recv[i].at[pl.ds(0, 31)], y_recv_sem.at[i])
                rows = ret_recv[i][...].reshape(512, width)
                total = dot(wgt_hi[a], rows) + dot(wgt_lo[a], rows)
                part[i][...] = total.astype(BF).reshape(4, TOK, width)
                part_recv[i][along[a]] = part[i][along[a]]
                for d in (1, 3, 2):
                    to = line_partner(a, x, y, z, d) + (c,)
                    remote(
                        part[i].at[lax.rem(along[a] + d, 4)],
                        part_recv[i].at[along[a]],
                        z_send_sem.at[i],
                        z_recv_sem.at[i],
                        to,
                    ).start()
    for i, (a, col, width, _) in enumerate(CHUNKS):
        wait_bytes(part_recv[i].at[pl.ds(0, 3)], z_recv_sem.at[i])
        total = hid[:, col : col + width]
        for s in range(4):
            total = total + part_recv[i][s].astype(F32)
        out_ref[:, col : col + width] = total.astype(BF)

    wait_bytes(b_buf.at[:, pl.ds(0, 896)], b_send_sem)
    wait_bytes(a_buf.at[pl.ds(0, 3)], a_send_sem)
    wait_bytes(c_recv.at[pl.ds(0, 15)], c_send_sem)
    wait_bytes(meta_all9(meta_all), m_send_sem)
    for i in range(n):
        wait_bytes(gath[i].at[pl.ds(0, 3)], g_send_sem.at[i])
        wait_bytes(slot_send[i].at[pl.ds(0, 31)], y_send_sem.at[i])
        wait_bytes(part[i].at[pl.ds(0, 3)], z_send_sem.at[i])


def meta_all9(meta_all):
    return meta_all.at[:, pl.ds(0, 3)]


def on_device(
    queries, keys, values, document_index, out_proj, residual_in, norm_gain, expert_ids, gate_weights, w_gate_up, w_down
):
    meta = jnp.concatenate([expert_ids.astype(F32).T, gate_weights.T], axis=0)
    meta = jnp.tile(meta, (1, 4))
    vmem = pl.BlockSpec(memory_space=pltpu.VMEM)
    hbm = pl.BlockSpec(memory_space=pl.ANY)
    dma = pltpu.SemaphoreType.DMA
    n = len(CHUNKS)

    def buf(*shape, dtype=BF):
        return pltpu.VMEM(shape, dtype)

    widths = [chunk[2] for chunk in CHUNKS]
    scratch = [
        buf(MODEL, 2 * FF),
        buf(FF, MODEL),
        buf(1024, 1024),
        buf(4, 128, 1024),
        buf(4, 128, 1024),
        buf(16, TOK, 1024),
        buf(TOK, MODEL, dtype=F32),
        buf(512, 2 * FF, dtype=F32),
        buf(512, FF),
        buf(2, 512, FF),
        buf(3, 4, 16, 128, dtype=F32),
        buf(3, 512, 128),
        buf(3, 128, 512),
        buf(3, 128, 512),
        buf(2, 256, 256),
        buf(2, 256, 256),
    ]
    scratch += [buf(4, TOK, w) for w in widths]
    for _ in range(3):
        scratch += [buf(32, 16, w) for w in widths]
    for _ in range(2):
        scratch += [buf(4, TOK, w) for w in widths]
    scratch += [
        dma((6,)), dma, dma((3,)), dma, dma, dma((3,)), dma, dma, dma, dma,
        dma((n,)), dma((n,)), dma((n,)), dma((n,)), dma((n,)), dma((n,)), dma((n,)), dma((n,)),
    ]
    return pl.pallas_call(
        kernel,
        out_shape=jax.ShapeDtypeStruct((TOK, MODEL), BF),
        in_specs=[vmem] * 8 + [hbm] * 2,
        out_specs=vmem,
        scratch_shapes=scratch,
        name="layer",
        compiler_params=pltpu.CompilerParams(
            collective_id=0, has_side_effects=True, vmem_limit_bytes=66_000_000
        ),
    )(
        queries, keys, values, document_index, out_proj, residual_in, norm_gain.reshape(1, -1), meta, w_gate_up, w_down
    )


def solution(mesh):
    both = P(("group", "tensor"), None)
    expert = P(("group", "tensor"), None, None)
    pair = P("group", "tensor")
    in_specs = (pair, pair, pair, P("group", None), P("tensor", "group"), both, P(), both, both, expert, expert)
    return jax.shard_map(on_device, mesh=mesh, in_specs=in_specs, out_specs=both, check_vma=False)
```

```python
import functools

import jax
import jax.numpy as jnp
from jax import lax
from jax.experimental import pallas as pl
from jax.experimental.pallas import tpu as pltpu
from jax.sharding import PartitionSpec as P

HEAD = 128
MODEL = 4096
FF = 768
TOK = 32
CHUNKS = (
    (1, 1280, 512, 0),
    (0, 0, 512, 0),
    (2, 2560, 512, 0),
    (1, 1792, 512, 1),
    (0, 512, 512, 1),
    (2, 3072, 512, 1),
    (1, 2304, 256, 2),
    (0, 1024, 256, 2),
    (2, 3584, 512, 2),
)
GROUPS = 3
BF = jnp.bfloat16
F32 = jnp.float32


def dot(a, b):
    return jnp.dot(a, b, preferred_element_type=F32)


def device(x, y, z, c):
    return {"group": (x * 4 + z) * 2 + c, "tensor": y}


def plane_index(a, x, y, z, c):
    if a == 0:
        return c * 16 + z * 4 + y
    if a == 1:
        return c * 16 + z * 4 + x
    return c * 16 + x * 4 + y


def plane_partner(a, x, y, z, c, k):
    nc = lax.rem(c + lax.rem(k, 2), 2)
    lo = lax.rem(k // 2, 4)
    hi = k // 8
    if a == 0:
        return x, lax.rem(y + lo, 4), lax.rem(z + hi, 4), nc
    if a == 1:
        return lax.rem(x + lo, 4), y, lax.rem(z + hi, 4), nc
    return lax.rem(x + hi, 4), lax.rem(y + lo, 4), z, nc


def line_partner(a, x, y, z, d):
    if a == 0:
        return lax.rem(x + d, 4), y, z
    if a == 1:
        return x, lax.rem(y + d, 4), z
    return x, y, lax.rem(z + d, 4)


def axis_row(a, canon):
    r = canon & 3
    y = (canon >> 2) & 3
    x = (canon >> 4) & 3
    z = (canon >> 6) & 3
    if a == 0:
        return z * 64 + y * 16 + x * 4 + r
    return x * 64 + y * 16 + z * 4 + r


def iota(shape, dim):
    return lax.broadcasted_iota(jnp.int32, shape, dim)


def kernel(
    q_ref, k_ref, v_ref, doc_ref, wo_ref, res_ref, gain_ref, ids_ref, gates_ref, w1_hbm, w2_hbm, out_ref, *scratch
):
    n = len(CHUNKS)
    (w1, w2, b_buf, a_buf, c_send, c_recv, hid, proj, act, act_p, meta, turn, meta_all, sel, wgt, perm, perm_t) = scratch[:17]
    rest = scratch[17:]
    gath, slot_send, slot_recv, ret_recv, part, part_recv = (rest[i * n : (i + 1) * n] for i in range(6))
    (
        w_sem, b_send_sem, b_recv_sem, b_sib_sem, a_send_sem, a_recv_sem, c_send_sem, c_recv_sem, m_send_sem, m_recv_sem,
        g_send_sem, g_recv_sem, s_send_sem, s_recv_sem, y_send_sem, y_recv_sem, z_send_sem, z_recv_sem,
    ) = rest[6 * n :]

    g = lax.axis_index("group")
    y = lax.axis_index("tensor")
    x = g // 8
    z = lax.rem(g // 2, 4)
    c = lax.rem(g, 2)
    me = (x, y, z, c)
    along = (x, y, z)

    def remote(src, dst, send, recv, to):
        return pltpu.make_async_remote_copy(
            src_ref=src, dst_ref=dst, send_sem=send, recv_sem=recv, device_id=device(*to)
        )

    def wait_bytes(ref, sem):
        pltpu.make_async_copy(ref, ref, sem).wait()

    barrier = pltpu.get_barrier_semaphore()

    def greet(to):
        pl.semaphore_signal(barrier, inc=1, device_id=device(*to))
        return 0

    def moved(dx, dy, dz, dc):
        return lax.rem(x + dx, 4), lax.rem(y + dy, 4), lax.rem(z + dz, 4), lax.rem(c + dc, 2)

    lax.fori_loop(1, 32, lambda k, _: greet(moved(k // 8, 0, lax.rem(k // 2, 4), lax.rem(k, 2))), 0)
    lax.fori_loop(8, 32, lambda k, _: greet(moved(0, k // 8, lax.rem(k // 2, 4), lax.rem(k, 2))), 0)
    lax.fori_loop(6, 24, lambda k, _: greet(moved(k // 6, 1 + lax.rem(k // 2, 3), 0, lax.rem(k, 2))), 0)

    loads = []
    for i in range(4):
        loads.append(
            pltpu.make_async_copy(w1_hbm.at[0, pl.ds(i * 1024, 1024)], w1.at[pl.ds(i * 1024, 1024)], w_sem.at[i])
        )
    for i in range(2):
        loads.append(
            pltpu.make_async_copy(w2_hbm.at[0, pl.ds(i * 384, 384)], w2.at[pl.ds(i * 384, 384)], w_sem.at[4 + i])
        )
    for copy in loads:
        copy.start()

    doc = jnp.broadcast_to(doc_ref[...].astype(F32), (128, 128))
    visible = (doc == doc.T) & (iota((128, 128), 0) >= iota((128, 128), 1))
    keys = k_ref[...]
    vals = v_ref[...]

    def attend(h):
        query = q_ref[:, h * HEAD : (h + 1) * HEAD]
        scores = lax.dot_general(query, keys, (((1,), (1,)), ((), ())), preferred_element_type=F32)
        scores = jnp.where(visible, scores * (1.0 / HEAD**0.5), -1e30)
        top = jnp.max(scores, axis=-1, keepdims=True)
        expo = jnp.where(visible, jnp.exp(scores - top), 0.0)
        weights = (expo / jnp.sum(expo, axis=-1, keepdims=True)).astype(BF)
        a_buf[z, :, h * HEAD : (h + 1) * HEAD] = dot(weights, vals).astype(BF)

    def send_heads(half):
        cols = pl.ds(half * 512, 512)
        for d in (1, 3, 2):
            to = (x, y, lax.rem(z + d, 4), c)
            remote(a_buf.at[z, :, cols], a_buf.at[z, :, cols], a_send_sem, a_recv_sem.at[d - 1], to).start()

    def b_cols(xx, cc):
        return pl.ds(pl.multiple_of((xx * 2 + cc) * 128, 128), 128)

    for s in range(4):
        turn[s * TOK : (s + 1) * TOK, 0:8] = ids_ref[...].astype(F32)
    meta[0:8] = turn[...].T[0:8]
    for s in range(4):
        turn[s * TOK : (s + 1) * TOK, 0:8] = gates_ref[...]
    meta[8:16] = turn[...].T[0:8]
    for h in range(4):
        attend(h)
    pl.semaphore_wait(barrier, 73)
    sibling = (x, y, z, 1 - c)
    remote(wo_ref, b_buf.at[:, b_cols(x, c)], b_send_sem, b_sib_sem.at[0], sibling).start()
    for d in (1, 3):
        to = (lax.rem(x + d, 4), y, z, c)
        remote(wo_ref, b_buf.at[:, b_cols(x, c)], b_send_sem, b_recv_sem.at[d - 1], to).start()
    for a in range(3):
        for d in (1, 3, 2):
            to = line_partner(a, x, y, z, d) + (c,)
            remote(meta, meta_all.at[a, along[a]], m_send_sem, m_recv_sem, to).start()
    to = (lax.rem(x + 2, 4), y, z, c)
    remote(wo_ref, b_buf.at[:, b_cols(x, c)], b_send_sem, b_recv_sem.at[1], to).start()
    send_heads(0)
    for h in range(4, 8):
        attend(h)
    send_heads(1)
    b_buf[:, b_cols(x, c)] = wo_ref[...]

    for a in range(3):
        meta_all[a, along[a]] = meta[...]
    canon = iota((256, 256), 0)
    canon_t = iota((256, 256), 1)
    for i, a in enumerate((0, 2)):
        perm[i] = (iota((256, 256), 1) == axis_row(a, canon)).astype(F32).astype(BF)
        perm_t[i] = (iota((256, 256), 0) == axis_row(a, canon_t)).astype(F32).astype(BF)
    wait_bytes(meta_all9(meta_all), m_recv_sem)
    lane = iota((128, 128), 1)
    row = iota((128, 128), 0)
    earlier = (((row >> 5) == (lane >> 5)) & (row < lane)).astype(F32).astype(BF)
    slot = iota((512, 128), 0)
    slot_lane = iota((512, 128), 1)
    for a in range(3):
        info = jnp.zeros((16, 128), F32)
        for s in range(4):
            info = jnp.where((iota((16, 128), 1) >> 5) == s, meta_all[a, s], info)
        named = jnp.zeros((128, 128), F32)
        gate = jnp.zeros((128, 128), F32)
        row_f = row.astype(F32)
        for k in range(8):
            hit = jnp.broadcast_to(info[k : k + 1], (128, 128)) == row_f
            named = jnp.where(hit, 1.0, named)
            gate = jnp.where(hit, jnp.broadcast_to(info[8 + k : 9 + k], (128, 128)), gate)
        place = dot(named.astype(BF), earlier)
        place = jnp.where(named > 0.5, place + 1.0, 0.0).astype(BF)
        gate_hi = gate.astype(BF)
        gate_lo = (gate - gate_hi.astype(F32)).astype(BF)
        j = slot >> 4
        jc, jh, jl = j >> 4, (j >> 2) & 3, j & 3
        if a == 0:
            ex, ey, ez = x, jl, jh
        elif a == 1:
            ex, ey, ez = jl, y, jh
        else:
            ex, ey, ez = jh, jl, z
        expert = ((ex * 4 + ez) * 2 + jc) * 4 + ey
        pick = (slot_lane == expert).astype(F32).astype(BF)
        match = (dot(pick, place) == ((slot & 3) + 1).astype(F32)) & ((slot_lane >> 5) == ((slot >> 2) & 3))
        sel[a] = jnp.where(match, 1.0, 0.0).astype(BF)
        wgt[a, 0:128] = jnp.where(match, dot(pick, gate_hi), 0.0).T.astype(BF)
        wgt[a, 128:256] = jnp.where(match, dot(pick, gate_lo), 0.0).T.astype(BF)

    def project(d, e):
        zz = lax.rem(z + 4 - d, 4)
        xx = lax.rem(x + 4 - e, 4)
        cols = pl.ds(pl.multiple_of(xx * 256, 256), 256)
        c_send[zz, :, cols] = dot(a_buf[zz], b_buf[:, cols]).astype(BF)
        for dy in (1, 3, 2, 0):
            yy = lax.rem(y + dy, 4)
            rows = pl.ds(pl.multiple_of(yy * TOK, TOK), TOK)
            if d or dy:
                remote(
                    c_send.at[zz, rows, cols], c_recv.at[y * 4 + z, :, cols], c_send_sem, c_recv_sem, (x, yy, zz, c)
                ).start()
            else:
                c_recv[y * 4 + z, :, cols] = c_send[zz, rows, cols]

    def columns_in(e):
        xx = lax.rem(x + 4 - e, 4)
        if e:
            block = b_buf.at[:, b_cols(xx, c)]
            wait_bytes(block, b_recv_sem.at[e - 1])
            remote(block, block, b_send_sem, b_sib_sem.at[e], sibling).start()

    def columns_ready(e):
        xx = lax.rem(x + 4 - e, 4)
        wait_bytes(b_buf.at[:, b_cols(xx, 1 - c)], b_sib_sem.at[e])

    def heads_ready(d):
        wait_bytes(a_buf.at[lax.rem(z + 4 - d, 4)], a_recv_sem.at[d - 1])

    columns_ready(0)
    project(0, 0)
    columns_in(1)
    columns_in(3)
    columns_ready(1)
    project(0, 1)
    columns_ready(3)
    project(0, 3)
    heads_ready(1)
    for e in (0, 1, 3):
        project(1, e)
    heads_ready(3)
    for e in (0, 1, 3):
        project(3, e)
    columns_in(2)
    columns_ready(2)
    for d in (0, 1, 3):
        project(d, 2)
    heads_ready(2)
    for e in (0, 1, 3, 2):
        project(2, e)
    wait_bytes(c_recv.at[pl.ds(0, 15)], c_recv_sem)
    square = jnp.zeros((TOK, 256), F32)
    for zz in range(4):
        for xx in range(4):
            col = (xx * 4 + zz) * 256
            value = res_ref[:, col : col + 256].astype(F32)
            for yy in range(4):
                value = value + c_recv[yy * 4 + zz, :, xx * 256 : (xx + 1) * 256].astype(F32)
            hid[:, col : col + 256] = value
            square = square + value * value
    scale = lax.rsqrt(jnp.sum(square, axis=-1, keepdims=True) * (1.0 / MODEL) + 1e-06)

    for i, (a, col, width, _) in enumerate(CHUNKS):
        normed = (hid[:, col : col + width] * scale * gain_ref[:, col : col + width]).astype(BF)
        gath[i][along[a]] = normed
        for d in (1, 3, 2):
            to = line_partner(a, x, y, z, d) + (c,)
            mine = gath[i].at[along[a]]
            remote(mine, mine, g_send_sem.at[i], g_recv_sem.at[i], to).start()

    def exchange(members, sources, targets, send_sem, recv_sem):
        def step(k, _):
            for i in members:
                a = CHUNKS[i][0]
                to = plane_partner(a, *me, k)
                remote(
                    sources[i].at[plane_index(a, *to)],
                    targets[i].at[plane_index(a, *me)],
                    send_sem.at[i],
                    recv_sem.at[i],
                    to,
                ).start()
            return 0

        lax.fori_loop(1, 32, step, 0)
        for i in members:
            mine = plane_index(CHUNKS[i][0], *me)
            targets[i][mine] = sources[i][mine]

    for group in range(GROUPS):
        for i, (a, col, width, grp) in enumerate(CHUNKS):
            if grp == group:
                wait_bytes(gath[i].at[pl.ds(0, 3)], g_recv_sem.at[i])
                rows = dot(sel[a], gath[i][...].reshape(128, width))
                slot_send[i][...] = rows.astype(BF).reshape(32, 16, width)
        members = [i for i in range(n) if CHUNKS[i][3] == group]
        exchange(members, slot_send, slot_recv, s_send_sem, s_recv_sem)

    for copy in loads:
        copy.wait()

    for group in range(GROUPS):
        members = [i for i in range(n) if CHUNKS[i][3] == group]
        for i in members:
            a, col, width, _ = CHUNKS[i]
            wait_bytes(slot_recv[i].at[pl.ds(0, 31)], s_recv_sem.at[i])
            if a != 1:
                for half in range(2):
                    block = slot_recv[i][half * 16 : half * 16 + 16].reshape(256, width)
                    moved = dot(perm[a // 2], block).astype(BF)
                    slot_recv[i][half * 16 : half * 16 + 16] = moved.reshape(16, 16, width)

        def up(t, _, members=members, group=group):
            cols = pl.ds(pl.multiple_of(t * 256, 256), 256)
            total = proj[:, cols] if group else jnp.zeros((512, 256), F32)
            for i in members:
                _, col, width, _ = CHUNKS[i]
                total = total + dot(slot_recv[i][...].reshape(512, width), w1[col : col + width, cols])
            proj[:, cols] = total
            return 0

        lax.fori_loop(0, 6, up, 0)

    def activate(t, _):
        rows = pl.ds(pl.multiple_of(t * 64, 64), 64)
        gate = proj[rows, :FF]
        act[rows, :] = (gate / (1.0 + jnp.exp(-gate)) * proj[rows, FF:]).astype(BF)
        return 0

    lax.fori_loop(0, 8, activate, 0)
    for i in range(2):
        for half in range(2):
            rows = slice(half * 256, half * 256 + 256)
            act_p[i, rows, :] = dot(perm_t[i], act[rows, :]).astype(BF)

    for i, (a, col, width, _) in enumerate(CHUNKS):
        wait_bytes(slot_send[i].at[pl.ds(0, 31)], s_send_sem.at[i])
        for t in range(0, width, 256):
            mine = act[...] if a == 1 else act_p[a // 2]
            rows = dot(mine, w2[:, col + t : col + t + 256]).astype(BF)
            slot_send[i][:, :, t : t + 256] = rows.reshape(32, 16, 256)
        exchange([i], slot_send, ret_recv, y_send_sem, y_recv_sem)

    for group in range(GROUPS):
        for i, (a, col, width, grp) in enumerate(CHUNKS):
            if grp == group:
                wait_bytes(ret_recv[i].at[pl.ds(0, 31)], y_recv_sem.at[i])
                rows = ret_recv[i][...].reshape(512, width)
                both = dot(wgt[a], rows)
                total = both[0:128] + both[128:256]
                part[i][...] = total.astype(BF).reshape(4, TOK, width)
                part_recv[i][along[a]] = part[i][along[a]]
                for d in (1, 3, 2):
                    to = line_partner(a, x, y, z, d) + (c,)
                    remote(
                        part[i].at[lax.rem(along[a] + d, 4)],
                        part_recv[i].at[along[a]],
                        z_send_sem.at[i],
                        z_recv_sem.at[i],
                        to,
                    ).start()
    for i, (a, col, width, _) in enumerate(CHUNKS):
        wait_bytes(part_recv[i].at[pl.ds(0, 3)], z_recv_sem.at[i])
        total = hid[:, col : col + width]
        for s in range(4):
            total = total + part_recv[i][s].astype(F32)
        out_ref[:, col : col + width] = total.astype(BF)

    wait_bytes(b_buf.at[:, pl.ds(0, 896)], b_send_sem)
    wait_bytes(a_buf.at[pl.ds(0, 3)], a_send_sem)
    wait_bytes(c_recv.at[pl.ds(0, 15)], c_send_sem)
    wait_bytes(meta_all9(meta_all), m_send_sem)
    for i in range(n):
        wait_bytes(gath[i].at[pl.ds(0, 3)], g_send_sem.at[i])
        wait_bytes(slot_send[i].at[pl.ds(0, 31)], y_send_sem.at[i])
        wait_bytes(part[i].at[pl.ds(0, 3)], z_send_sem.at[i])


def meta_all9(meta_all):
    return meta_all.at[:, pl.ds(0, 3)]


def on_device(
    queries, keys, values, document_index, out_proj, residual_in, norm_gain, expert_ids, gate_weights, w_gate_up, w_down
):
    vmem = pl.BlockSpec(memory_space=pltpu.VMEM)
    hbm = pl.BlockSpec(memory_space=pl.ANY)
    dma = pltpu.SemaphoreType.DMA
    n = len(CHUNKS)

    def buf(*shape, dtype=BF):
        return pltpu.VMEM(shape, dtype)

    widths = [chunk[2] for chunk in CHUNKS]
    scratch = [
        buf(MODEL, 2 * FF),
        buf(FF, MODEL),
        buf(1024, 1024),
        buf(4, 128, 1024),
        buf(4, 128, 1024),
        buf(16, TOK, 1024),
        buf(TOK, MODEL, dtype=F32),
        buf(512, 2 * FF, dtype=F32),
        buf(512, FF),
        buf(2, 512, FF),
        buf(16, 128, dtype=F32),
        buf(128, 128, dtype=F32),
        buf(3, 4, 16, 128, dtype=F32),
        buf(3, 512, 128),
        buf(3, 256, 512),
        buf(2, 256, 256),
        buf(2, 256, 256),
    ]
    scratch += [buf(4, TOK, w) for w in widths]
    for _ in range(3):
        scratch += [buf(32, 16, w) for w in widths]
    for _ in range(2):
        scratch += [buf(4, TOK, w) for w in widths]
    scratch += [
        dma((6,)), dma, dma((3,)), dma((4,)), dma, dma((3,)), dma, dma, dma, dma,
        dma((n,)), dma((n,)), dma((n,)), dma((n,)), dma((n,)), dma((n,)), dma((n,)), dma((n,)),
    ]
    return pl.pallas_call(
        kernel,
        out_shape=jax.ShapeDtypeStruct((TOK, MODEL), BF),
        in_specs=[vmem] * 9 + [hbm] * 2,
        out_specs=vmem,
        scratch_shapes=scratch,
        name="layer",
        compiler_params=pltpu.CompilerParams(
            collective_id=0, has_side_effects=True, vmem_limit_bytes=66_000_000
        ),
    )(
        queries, keys, values, document_index, out_proj, residual_in, norm_gain.reshape(1, -1), expert_ids, gate_weights,
        w_gate_up, w_down
    )


def solution(mesh):
    both = P(("group", "tensor"), None)
    expert = P(("group", "tensor"), None, None)
    pair = P("group", "tensor")
    in_specs = (pair, pair, pair, P("group", None), P("tensor", "group"), both, P(), both, both, expert, expert)
    return jax.shard_map(on_device, mesh=mesh, in_specs=in_specs, out_specs=both, check_vma=False)
```

```python
import functools

import jax
import jax.numpy as jnp
from jax import lax
from jax.experimental import pallas as pl
from jax.experimental.pallas import tpu as pltpu
from jax.sharding import PartitionSpec as P

HEAD = 128
MODEL = 4096
FF = 768
TOK = 32
CHUNKS = (
    (1, 1280, 512, 0),
    (0, 0, 512, 0),
    (2, 2560, 512, 0),
    (1, 1792, 512, 1),
    (0, 512, 512, 1),
    (2, 3072, 512, 1),
    (1, 2304, 256, 2),
    (0, 1024, 256, 2),
    (2, 3584, 512, 2),
)
GROUPS = 3
BF = jnp.bfloat16
F32 = jnp.float32


def dot(a, b):
    return jnp.dot(a, b, preferred_element_type=F32)


def device(x, y, z, c):
    return {"group": (x * 4 + z) * 2 + c, "tensor": y}


def plane_index(a, x, y, z, c):
    if a == 0:
        return c * 16 + z * 4 + y
    if a == 1:
        return c * 16 + z * 4 + x
    return c * 16 + x * 4 + y


def plane_partner(a, x, y, z, c, k):
    nc = lax.rem(c + lax.rem(k, 2), 2)
    lo = lax.rem(k // 2, 4)
    hi = k // 8
    if a == 0:
        return x, lax.rem(y + lo, 4), lax.rem(z + hi, 4), nc
    if a == 1:
        return lax.rem(x + lo, 4), y, lax.rem(z + hi, 4), nc
    return lax.rem(x + hi, 4), lax.rem(y + lo, 4), z, nc


def line_partner(a, x, y, z, d):
    if a == 0:
        return lax.rem(x + d, 4), y, z
    if a == 1:
        return x, lax.rem(y + d, 4), z
    return x, y, lax.rem(z + d, 4)


def axis_row(a, canon):
    r = canon & 3
    y = (canon >> 2) & 3
    x = (canon >> 4) & 3
    z = (canon >> 6) & 3
    if a == 0:
        return z * 64 + y * 16 + x * 4 + r
    return x * 64 + y * 16 + z * 4 + r


def iota(shape, dim):
    return lax.broadcasted_iota(jnp.int32, shape, dim)


def kernel(
    *refs
):
    n = len(CHUNKS)
    operands, (w1_hbm, w2_hbm, out_ref), inputs, scratch = refs[:9], refs[9:12], refs[12:21], refs[21:]
    q_ref, k_ref, v_ref, doc_ref, ids_ref, gates_ref, wo_ref, gain_ref, res_ref = inputs
    (w1, w2, b_buf, a_buf, c_send, c_recv, hid, proj, act, act_p, meta, turn, meta_all, sel, wgt, perm, perm_t) = scratch[:17]
    rest = scratch[17:]
    gath, slot_send, slot_recv, ret_recv, part, part_recv = (rest[i * n : (i + 1) * n] for i in range(6))
    (
        in_sem, w_sem, b_send_sem, b_recv_sem, b_sib_sem, a_send_sem, a_recv_sem, c_send_sem, c_recv_sem, m_send_sem, m_recv_sem,
        g_send_sem, g_recv_sem, s_send_sem, s_recv_sem, y_send_sem, y_recv_sem, z_send_sem, z_recv_sem,
    ) = rest[6 * n :]

    g = lax.axis_index("group")
    y = lax.axis_index("tensor")
    x = g // 8
    z = lax.rem(g // 2, 4)
    c = lax.rem(g, 2)
    me = (x, y, z, c)
    along = (x, y, z)

    def remote(src, dst, send, recv, to):
        return pltpu.make_async_remote_copy(
            src_ref=src, dst_ref=dst, send_sem=send, recv_sem=recv, device_id=device(*to)
        )

    def wait_bytes(ref, sem):
        pltpu.make_async_copy(ref, ref, sem).wait()

    takes = [pltpu.make_async_copy(src, dst, in_sem.at[i]) for i, (src, dst) in enumerate(zip(operands, inputs))]
    for copy in takes:
        copy.start()
    barrier = pltpu.get_barrier_semaphore()

    def greet(to):
        pl.semaphore_signal(barrier, inc=1, device_id=device(*to))
        return 0

    lax.fori_loop(1, 4, lambda k, _: greet((lax.rem(x + k, 4), y, z, c)), 0)
    greet((x, y, z, 1 - c))
    lax.fori_loop(1, 16, lambda k, _: greet((x, lax.rem(y + k // 4, 4), lax.rem(z + k, 4), c)), 0)

    for copy in takes[:6]:
        copy.wait()
    doc = jnp.broadcast_to(doc_ref[...].astype(F32), (128, 128))
    visible = (doc == doc.T) & (iota((128, 128), 0) >= iota((128, 128), 1))
    keys = k_ref[...]
    vals = v_ref[...]

    def attend(h):
        query = q_ref[:, h * HEAD : (h + 1) * HEAD]
        scores = lax.dot_general(query, keys, (((1,), (1,)), ((), ())), preferred_element_type=F32)
        scores = jnp.where(visible, scores * (1.0 / HEAD**0.5), -1e30)
        top = jnp.max(scores, axis=-1, keepdims=True)
        expo = jnp.where(visible, jnp.exp(scores - top), 0.0)
        weights = (expo / jnp.sum(expo, axis=-1, keepdims=True)).astype(BF)
        a_buf[z, :, h * HEAD : (h + 1) * HEAD] = dot(weights, vals).astype(BF)

    def send_heads(half):
        cols = pl.ds(half * 512, 512)
        for d in (1, 3):
            to = (x, y, lax.rem(z + d, 4), c)
            remote(a_buf.at[z, :, cols], a_buf.at[z, :, cols], a_send_sem, a_recv_sem.at[d - 1], to).start()

    def b_cols(xx, cc):
        return pl.ds(pl.multiple_of((xx * 2 + cc) * 128, 128), 128)

    lanes = iota((8, 128), 1)
    for i, ref in enumerate((ids_ref, gates_ref)):
        turn[:, 0:TOK] = ref[...].astype(F32)
        once = jnp.where(lanes < TOK, turn[...], 0.0)
        meta[8 * i : 8 * i + 8] = once + sum(pltpu.roll(once, TOK * s, 1) for s in (1, 2, 3))
    for h in range(4):
        attend(h)
    takes[6].wait()
    pl.semaphore_wait(barrier, 19)
    sibling = (x, y, z, 1 - c)
    for a in range(3):
        for d in (1, 3, 2):
            to = line_partner(a, x, y, z, d) + (c,)
            remote(meta, meta_all.at[a, along[a]], m_send_sem, m_recv_sem, to).start()
    remote(wo_ref, b_buf.at[:, b_cols(x, c)], b_send_sem, b_sib_sem.at[0], sibling).start()
    for d in (1, 3):
        to = (lax.rem(x + d, 4), y, z, c)
        remote(wo_ref, b_buf.at[:, b_cols(x, c)], b_send_sem, b_recv_sem.at[d - 1], to).start()
    send_heads(0)
    loads = []
    for i in range(4):
        loads.append(
            pltpu.make_async_copy(w1_hbm.at[0, pl.ds(i * 1024, 1024)], w1.at[pl.ds(i * 1024, 1024)], w_sem.at[i])
        )
    for i in range(2):
        loads.append(
            pltpu.make_async_copy(w2_hbm.at[0, pl.ds(i * 384, 384)], w2.at[pl.ds(i * 384, 384)], w_sem.at[4 + i])
        )
    for copy in loads:
        copy.start()

    for h in range(4, 8):
        attend(h)
    send_heads(1)
    b_buf[:, b_cols(x, c)] = wo_ref[...]

    for a in range(3):
        meta_all[a, along[a]] = meta[...]
    canon = iota((256, 256), 0)
    canon_t = iota((256, 256), 1)
    for i, a in enumerate((0, 2)):
        perm[i] = (iota((256, 256), 1) == axis_row(a, canon)).astype(F32).astype(BF)
        perm_t[i] = (iota((256, 256), 0) == axis_row(a, canon_t)).astype(F32).astype(BF)
    wait_bytes(meta_all9(meta_all), m_recv_sem)
    lane = iota((128, 128), 1)
    row = iota((128, 128), 0)
    earlier = (((row >> 5) == (lane >> 5)) & (row < lane)).astype(F32).astype(BF)
    slot = iota((512, 128), 0)
    slot_lane = iota((512, 128), 1)
    for a in range(3):
        info = jnp.zeros((16, 128), F32)
        for s in range(4):
            info = jnp.where((iota((16, 128), 1) >> 5) == s, meta_all[a, s], info)
        named = jnp.zeros((128, 128), F32)
        gate = jnp.zeros((128, 128), F32)
        row_f = row.astype(F32)
        for k in range(8):
            hit = jnp.broadcast_to(info[k : k + 1], (128, 128)) == row_f
            named = jnp.where(hit, 1.0, named)
            gate = jnp.where(hit, jnp.broadcast_to(info[8 + k : 9 + k], (128, 128)), gate)
        place = dot(named.astype(BF), earlier)
        place = jnp.where(named > 0.5, place + 1.0, 0.0).astype(BF)
        gate_hi = gate.astype(BF)
        gate_lo = (gate - gate_hi.astype(F32)).astype(BF)
        j = slot >> 4
        jc, jh, jl = j >> 4, (j >> 2) & 3, j & 3
        if a == 0:
            ex, ey, ez = x, jl, jh
        elif a == 1:
            ex, ey, ez = jl, y, jh
        else:
            ex, ey, ez = jh, jl, z
        expert = ((ex * 4 + ez) * 2 + jc) * 4 + ey
        pick = (slot_lane == expert).astype(F32).astype(BF)
        match = (dot(pick, place) == ((slot & 3) + 1).astype(F32)) & ((slot_lane >> 5) == ((slot >> 2) & 3))
        sel[a] = jnp.where(match, 1.0, 0.0).astype(BF)
        wgt[a, 0:128] = jnp.where(match, dot(pick, gate_hi), 0.0).T.astype(BF)
        wgt[a, 128:256] = jnp.where(match, dot(pick, gate_lo), 0.0).T.astype(BF)

    def project(d, e):
        zz = lax.rem(z + 4 - d, 4)
        xx = lax.rem(x + 4 - e, 4)
        cols = pl.ds(pl.multiple_of(xx * 256, 256), 256)
        c_send[zz, :, cols] = dot(a_buf[zz], b_buf[:, cols]).astype(BF)
        for dy in (1, 3, 2, 0):
            yy = lax.rem(y + dy, 4)
            rows = pl.ds(pl.multiple_of(yy * TOK, TOK), TOK)
            if d or dy:
                remote(
                    c_send.at[zz, rows, cols], c_recv.at[y * 4 + z, :, cols], c_send_sem, c_recv_sem, (x, yy, zz, c)
                ).start()
            else:
                c_recv[y * 4 + z, :, cols] = c_send[zz, rows, cols]

    def columns_in(e):
        xx = lax.rem(x + 4 - e, 4)
        if e:
            block = b_buf.at[:, b_cols(xx, c)]
            wait_bytes(block, b_recv_sem.at[e - 1])
            remote(block, block, b_send_sem, b_sib_sem.at[e], sibling).start()
        if e in (1, 3):
            half = b_buf.at[pl.ds(0 if e == 1 else 512, 512), b_cols(xx, c)]
            remote(half, half, b_send_sem, b_recv_sem.at[1], (lax.rem(x + e, 4), y, z, c)).start()

    def columns_ready(e):
        xx = lax.rem(x + 4 - e, 4)
        wait_bytes(b_buf.at[:, b_cols(xx, 1 - c)], b_sib_sem.at[e])

    def heads_ready(d):
        zz = lax.rem(z + 4 - d, 4)
        wait_bytes(a_buf.at[zz], a_recv_sem.at[d - 1])
        if d in (1, 3):
            half = a_buf.at[zz, :, pl.ds(0 if d == 1 else 512, 512)]
            remote(half, half, a_send_sem, a_recv_sem.at[1], (x, y, lax.rem(z + d, 4), c)).start()

    columns_ready(0)
    project(0, 0)
    columns_in(1)
    columns_in(3)
    heads_ready(1)
    heads_ready(3)
    columns_ready(1)
    columns_ready(3)
    for e in (1, 3):
        project(0, e)
    for d in (1, 3):
        for e in (0, 1, 3):
            project(d, e)
    columns_in(2)
    columns_ready(2)
    for d in (0, 1, 3):
        project(d, 2)
    heads_ready(2)
    for e in (0, 1, 3, 2):
        project(2, e)
    wait_bytes(c_recv.at[pl.ds(0, 15)], c_recv_sem)
    for copy in takes[7:]:
        copy.wait()
    square = jnp.zeros((TOK, 256), F32)
    for zz in range(4):
        for xx in range(4):
            col = (xx * 4 + zz) * 256
            value = res_ref[:, col : col + 256].astype(F32)
            for yy in range(4):
                value = value + c_recv[yy * 4 + zz, :, xx * 256 : (xx + 1) * 256].astype(F32)
            hid[:, col : col + 256] = value
            square = square + value * value
    scale = lax.rsqrt(jnp.sum(square, axis=-1, keepdims=True) * (1.0 / MODEL) + 1e-06)

    for i, (a, col, width, _) in enumerate(CHUNKS):
        normed = (hid[:, col : col + width] * scale * gain_ref[:, col : col + width]).astype(BF)
        gath[i][along[a]] = normed
        for d in (1, 3, 2):
            to = line_partner(a, x, y, z, d) + (c,)
            mine = gath[i].at[along[a]]
            remote(mine, mine, g_send_sem.at[i], g_recv_sem.at[i], to).start()

    def exchange(members, sources, targets, send_sem, recv_sem, core):
        def put(i, to):
            a = CHUNKS[i][0]
            remote(
                sources[i].at[plane_index(a, *to)],
                targets[i].at[plane_index(a, *me)],
                send_sem.at[i],
                recv_sem.at[i],
                to,
            ).start()

        def step(k, _):
            for i in members:
                px, py, pz, _c = plane_partner(CHUNKS[i][0], x, y, z, c, k * 2)
                put(i, (px, py, pz, core))
            return 0

        lax.fori_loop(1, 16, step, 0)
        if core == 0:
            for i in members:
                put(i, sibling)
                mine = plane_index(CHUNKS[i][0], *me)
                targets[i][mine] = sources[i][mine]

    for group in range(GROUPS):
        for i in range(n):
            if CHUNKS[i][3] == group:
                wait_bytes(gath[i].at[pl.ds(0, 3)], g_recv_sem.at[i])
        for i, (a, col, width, grp) in enumerate(CHUNKS):
            if grp == group:
                rows = dot(sel[a], gath[i][...].reshape(128, width))
                slot_send[i][...] = rows.astype(BF).reshape(32, 16, width)
        members = [i for i in range(n) if CHUNKS[i][3] == group]
        exchange(members, slot_send, slot_recv, s_send_sem, s_recv_sem, 0)
    for group in range(GROUPS):
        members = [i for i in range(n) if CHUNKS[i][3] == group]
        exchange(members, slot_send, slot_recv, s_send_sem, s_recv_sem, 1)

    for copy in loads:
        copy.wait()

    for group in range(GROUPS):
        members = [i for i in range(n) if CHUNKS[i][3] == group]
        for i in members:
            a, col, width, _ = CHUNKS[i]
            wait_bytes(slot_recv[i].at[pl.ds(0, 31)], s_recv_sem.at[i])
            if a != 1:
                for half in range(2):
                    block = slot_recv[i][half * 16 : half * 16 + 16].reshape(256, width)
                    moved = dot(perm[a // 2], block).astype(BF)
                    slot_recv[i][half * 16 : half * 16 + 16] = moved.reshape(16, 16, width)

        def gather_up(cols, members=members, group=group):
            total = proj[:, cols] if group else jnp.zeros((512, 256), F32)
            for i in members:
                _, col, width, _ = CHUNKS[i]
                total = total + dot(slot_recv[i][...].reshape(512, width), w1[col : col + width, cols])
            return total

        def up(t, _, gather_up=gather_up):
            cols = pl.ds(pl.multiple_of(t * 256, 256), 256)
            proj[:, cols] = gather_up(cols)
            return 0

        def last(t, _, gather_up=gather_up):
            first = pl.multiple_of(t * 256, 256)
            gate = gather_up(pl.ds(first, 256))
            value = gather_up(pl.ds(pl.multiple_of(first + FF, 256), 256))
            act[:, pl.ds(first, 256)] = (gate / (1.0 + jnp.exp(-gate)) * value).astype(BF)
            return 0

        if group < GROUPS - 1:
            lax.fori_loop(0, 6, up, 0)
        else:
            lax.fori_loop(0, 3, last, 0)

    for i in range(2):
        for half in range(2):
            rows = slice(half * 256, half * 256 + 256)
            act_p[i, rows, :] = dot(perm_t[i], act[rows, :]).astype(BF)

    for i, (a, col, width, _) in enumerate(CHUNKS):
        wait_bytes(slot_send[i].at[pl.ds(0, 31)], s_send_sem.at[i])
        for t in range(0, width, 256):
            mine = act[...] if a == 1 else act_p[a // 2]
            rows = dot(mine, w2[:, col + t : col + t + 256]).astype(BF)
            slot_send[i][:, :, t : t + 256] = rows.reshape(32, 16, 256)
        for core in range(2):
            exchange([i], slot_send, ret_recv, y_send_sem, y_recv_sem, core)

    for group in range(GROUPS):
        for i, (a, col, width, grp) in enumerate(CHUNKS):
            if grp == group:
                wait_bytes(ret_recv[i].at[pl.ds(0, 31)], y_recv_sem.at[i])
                rows = ret_recv[i][...].reshape(512, width)
                both = dot(wgt[a], rows)
                total = both[0:128] + both[128:256]
                part[i][...] = total.astype(BF).reshape(4, TOK, width)
                part_recv[i][along[a]] = part[i][along[a]]
                for d in (1, 3, 2):
                    to = line_partner(a, x, y, z, d) + (c,)
                    remote(
                        part[i].at[lax.rem(along[a] + d, 4)],
                        part_recv[i].at[along[a]],
                        z_send_sem.at[i],
                        z_recv_sem.at[i],
                        to,
                    ).start()
    for i, (a, col, width, _) in enumerate(CHUNKS):
        wait_bytes(part_recv[i].at[pl.ds(0, 3)], z_recv_sem.at[i])
        total = hid[:, col : col + width]
        for s in range(4):
            total = total + part_recv[i][s].astype(F32)
        out_ref[:, col : col + width] = total.astype(BF)

    wait_bytes(b_buf.at[:, pl.ds(0, 896)], b_send_sem)
    wait_bytes(a_buf.at[pl.ds(0, 3)], a_send_sem)
    wait_bytes(c_recv.at[pl.ds(0, 15)], c_send_sem)
    wait_bytes(meta_all9(meta_all), m_send_sem)
    for i in range(n):
        wait_bytes(gath[i].at[pl.ds(0, 3)], g_send_sem.at[i])
        wait_bytes(slot_send[i].at[pl.ds(0, 31)], y_send_sem.at[i])
        wait_bytes(part[i].at[pl.ds(0, 3)], z_send_sem.at[i])


def meta_all9(meta_all):
    return meta_all.at[:, pl.ds(0, 3)]


def on_device(
    queries, keys, values, document_index, out_proj, residual_in, norm_gain, expert_ids, gate_weights, w_gate_up, w_down
):
    vmem = pl.BlockSpec(memory_space=pltpu.VMEM)
    hbm = pl.BlockSpec(memory_space=pl.ANY)
    dma = pltpu.SemaphoreType.DMA
    n = len(CHUNKS)

    def buf(*shape, dtype=BF):
        return pltpu.VMEM(shape, dtype)

    widths = [chunk[2] for chunk in CHUNKS]
    operands = (
        queries, keys, values, document_index, expert_ids.T, gate_weights.T, out_proj, norm_gain.reshape(1, -1), residual_in
    )
    scratch = [pltpu.VMEM(value.shape, value.dtype) for value in operands]
    scratch += [
        buf(MODEL, 2 * FF),
        buf(FF, MODEL),
        buf(1024, 1024),
        buf(4, 128, 1024),
        buf(4, 128, 1024),
        buf(16, TOK, 1024),
        buf(TOK, MODEL, dtype=F32),
        buf(512, 2 * FF, dtype=F32),
        buf(512, FF),
        buf(2, 512, FF),
        buf(16, 128, dtype=F32),
        buf(8, 128, dtype=F32),
        buf(3, 4, 16, 128, dtype=F32),
        buf(3, 512, 128),
        buf(3, 256, 512),
        buf(2, 256, 256),
        buf(2, 256, 256),
    ]
    scratch += [buf(4, TOK, w) for w in widths]
    for _ in range(3):
        scratch += [buf(32, 16, w) for w in widths]
    for _ in range(2):
        scratch += [buf(4, TOK, w) for w in widths]
    scratch += [
        dma((9,)), dma((6,)), dma, dma((3,)), dma((4,)), dma, dma((3,)), dma, dma, dma, dma,
        dma((n,)), dma((n,)), dma((n,)), dma((n,)), dma((n,)), dma((n,)), dma((n,)), dma((n,)),
    ]
    out = pl.pallas_call(
        kernel,
        out_shape=jax.ShapeDtypeStruct((TOK, MODEL), BF),
        in_specs=[hbm] * 11,
        out_specs=vmem,
        scratch_shapes=scratch,
        name="layer",
        compiler_params=pltpu.CompilerParams(
            collective_id=0, has_side_effects=True, vmem_limit_bytes=60_000_000
        ),
    )(*operands, w_gate_up, w_down)
    return out


def solution(mesh):
    both = P(("group", "tensor"), None)
    expert = P(("group", "tensor"), None, None)
    pair = P("group", "tensor")
    in_specs = (pair, pair, pair, P("group", None), P("tensor", "group"), both, P(), both, both, expert, expert)
    return jax.shard_map(on_device, mesh=mesh, in_specs=in_specs, out_specs=both, check_vma=False)
```

```python
import functools

import jax
import jax.numpy as jnp
from jax import lax
from jax.experimental import pallas as pl
from jax.experimental.pallas import tpu as pltpu
from jax.sharding import PartitionSpec as P

HEAD = 128
MODEL = 4096
FF = 768
TOK = 32
CHUNKS = (
    (1, 1280, 512, 0),
    (0, 0, 512, 0),
    (2, 2560, 512, 0),
    (1, 1792, 512, 1),
    (0, 512, 512, 1),
    (2, 3072, 512, 1),
    (1, 2304, 256, 2),
    (0, 1024, 256, 2),
    (2, 3584, 512, 2),
)
GROUPS = 3
BF = jnp.bfloat16
F32 = jnp.float32


def dot(a, b):
    return jnp.dot(a, b, preferred_element_type=F32)


def device(x, y, z, c):
    return {"group": (x * 4 + z) * 2 + c, "tensor": y}


def plane_index(a, x, y, z, c):
    if a == 0:
        return c * 16 + z * 4 + y
    if a == 1:
        return c * 16 + z * 4 + x
    return c * 16 + x * 4 + y


def plane_partner(a, x, y, z, c, k):
    nc = lax.rem(c + lax.rem(k, 2), 2)
    lo = lax.rem(k // 2, 4)
    hi = k // 8
    if a == 0:
        return x, lax.rem(y + lo, 4), lax.rem(z + hi, 4), nc
    if a == 1:
        return lax.rem(x + lo, 4), y, lax.rem(z + hi, 4), nc
    return lax.rem(x + hi, 4), lax.rem(y + lo, 4), z, nc


def line_partner(a, x, y, z, d):
    if a == 0:
        return lax.rem(x + d, 4), y, z
    if a == 1:
        return x, lax.rem(y + d, 4), z
    return x, y, lax.rem(z + d, 4)


def axis_row(a, canon):
    r = canon & 3
    y = (canon >> 2) & 3
    x = (canon >> 4) & 3
    z = (canon >> 6) & 3
    if a == 0:
        return z * 64 + y * 16 + x * 4 + r
    return x * 64 + y * 16 + z * 4 + r


def iota(shape, dim):
    return lax.broadcasted_iota(jnp.int32, shape, dim)


def kernel(
    *refs
):
    n = len(CHUNKS)
    operands, (w1_hbm, w2_hbm, out_ref), inputs, scratch = refs[:9], refs[9:12], refs[12:21], refs[21:]
    q_ref, k_ref, v_ref, doc_ref, ids_ref, gates_ref, wo_ref, gain_ref, res_ref = inputs
    (w1, w2, b_buf, a_buf, c_send, c_recv, hid, proj, act, act_p, meta, turn, meta_all, sel, wgt, perm, perm_t) = scratch[:17]
    rest = scratch[17:]
    gath, slot_send, slot_recv, ret_recv, part, part_recv = (rest[i * n : (i + 1) * n] for i in range(6))
    (
        turn_sem, in_sem, w_sem, b_send_sem, b_recv_sem, b_sib_sem, a_send_sem, a_recv_sem, c_send_sem, c_recv_sem, m_send_sem, m_recv_sem,
        g_send_sem, g_recv_sem, s_send_sem, s_recv_sem, y_send_sem, y_recv_sem, z_send_sem, z_recv_sem,
    ) = rest[6 * n :]

    g = lax.axis_index("group")
    y = lax.axis_index("tensor")
    x = g // 8
    z = lax.rem(g // 2, 4)
    c = lax.rem(g, 2)
    me = (x, y, z, c)
    along = (x, y, z)

    def remote(src, dst, send, recv, to):
        return pltpu.make_async_remote_copy(
            src_ref=src, dst_ref=dst, send_sem=send, recv_sem=recv, device_id=device(*to)
        )

    def wait_bytes(ref, sem):
        pltpu.make_async_copy(ref, ref, sem).wait()

    takes = [pltpu.make_async_copy(src, dst, in_sem.at[i]) for i, (src, dst) in enumerate(zip(operands, inputs))]
    for copy in takes:
        copy.start()
    barrier = pltpu.get_barrier_semaphore()

    def greet(to):
        pl.semaphore_signal(barrier, inc=1, device_id=device(*to))
        return 0

    lax.fori_loop(1, 4, lambda k, _: greet((lax.rem(x + k, 4), y, z, c)), 0)
    greet((x, y, z, 1 - c))
    lax.fori_loop(1, 16, lambda k, _: greet((x, lax.rem(y + k // 4, 4), lax.rem(z + k, 4), c)), 0)

    for copy in takes[:6]:
        copy.wait()
    doc = jnp.broadcast_to(doc_ref[...].astype(F32), (128, 128))
    visible = (doc == doc.T) & (iota((128, 128), 0) >= iota((128, 128), 1))
    keys = k_ref[...]
    vals = v_ref[...]

    def attend(h):
        query = q_ref[:, h * HEAD : (h + 1) * HEAD]
        scores = lax.dot_general(query, keys, (((1,), (1,)), ((), ())), preferred_element_type=F32)
        scores = jnp.where(visible, scores * (1.0 / HEAD**0.5), -1e30)
        top = jnp.max(scores, axis=-1, keepdims=True)
        expo = jnp.where(visible, jnp.exp(scores - top), 0.0)
        weights = (expo / jnp.sum(expo, axis=-1, keepdims=True)).astype(BF)
        a_buf[z, :, h * HEAD : (h + 1) * HEAD] = dot(weights, vals).astype(BF)

    def send_heads(d, pair):
        cols = pl.ds(pair * 256, 256)
        to = (x, y, lax.rem(z + d, 4), c)
        remote(a_buf.at[z, :, cols], a_buf.at[z, :, cols], a_send_sem, a_recv_sem.at[d - 1, pair], to).start()

    def b_cols(xx, cc):
        return pl.ds(pl.multiple_of((xx * 2 + cc) * 128, 128), 128)

    lanes = iota((8, 128), 1)
    for i, ref in enumerate((ids_ref, gates_ref)):
        turn[:, 0:TOK] = ref[...].astype(F32)
        once = jnp.where(lanes < TOK, turn[...], 0.0)
        meta[8 * i : 8 * i + 8] = once + sum(pltpu.roll(once, TOK * s, 1) for s in (1, 2, 3))
    for h in range(2):
        attend(h)
    takes[6].wait()
    pl.semaphore_wait(barrier, 19)
    sibling = (x, y, z, 1 - c)
    for a in range(3):
        for d in (1, 3, 2):
            to = line_partner(a, x, y, z, d) + (c,)
            remote(meta, meta_all.at[a, along[a]], m_send_sem, m_recv_sem, to).start()
    remote(wo_ref, b_buf.at[:, b_cols(x, c)], b_send_sem, b_sib_sem.at[0], sibling).start()
    for d, halves in ((1, (0, 1)), (3, (1, 0))):
        for half in halves:
            rows = pl.ds(half * 512, 512)
            to = (lax.rem(x + d, 4), y, z, c)
            remote(
                wo_ref.at[rows, :], b_buf.at[rows, b_cols(x, c)], b_send_sem, b_recv_sem.at[d - 1, half], to
            ).start()

    @pl.when(c == 0)
    def _():
        send_heads(1, 0)
        send_heads(3, 0)

    loads = []
    for i in range(4):
        loads.append(
            pltpu.make_async_copy(w1_hbm.at[0, pl.ds(i * 1024, 1024)], w1.at[pl.ds(i * 1024, 1024)], w_sem.at[i])
        )
    for i in range(2):
        loads.append(
            pltpu.make_async_copy(w2_hbm.at[0, pl.ds(i * 384, 384)], w2.at[pl.ds(i * 384, 384)], w_sem.at[4 + i])
        )
    for copy in loads:
        copy.start()

    for pair in range(1, 4):
        for h in (2 * pair, 2 * pair + 1):
            attend(h)

        @pl.when(c == 0)
        def _(pair=pair):
            send_heads(1, pair)
            if pair > 1:
                send_heads(3, pair)

    @pl.when(c == 0)
    def _():
        send_heads(3, 1)

    @pl.when(c == 1)
    def _():
        for up, down in ((0, 2), (1, 3), (2, 0), (3, 1)):
            send_heads(1, up)
            send_heads(3, down)

    b_buf[:, b_cols(x, c)] = wo_ref[...]

    for a in range(3):
        meta_all[a, along[a]] = meta[...]
    canon = iota((256, 256), 0)
    canon_t = iota((256, 256), 1)
    for i, a in enumerate((0, 2)):
        perm[i] = (iota((256, 256), 1) == axis_row(a, canon)).astype(F32).astype(BF)
        perm_t[i] = (iota((256, 256), 0) == axis_row(a, canon_t)).astype(F32).astype(BF)
    wait_bytes(meta_all9(meta_all), m_recv_sem)
    lane = iota((128, 128), 1)
    row = iota((128, 128), 0)
    earlier = (((row >> 5) == (lane >> 5)) & (row < lane)).astype(F32).astype(BF)
    slot = iota((512, 128), 0)
    slot_lane = iota((512, 128), 1)
    for a in range(3):
        info = jnp.zeros((16, 128), F32)
        for s in range(4):
            info = jnp.where((iota((16, 128), 1) >> 5) == s, meta_all[a, s], info)
        named = jnp.zeros((128, 128), F32)
        gate = jnp.zeros((128, 128), F32)
        row_f = row.astype(F32)
        for k in range(8):
            hit = jnp.broadcast_to(info[k : k + 1], (128, 128)) == row_f
            named = jnp.where(hit, 1.0, named)
            gate = jnp.where(hit, jnp.broadcast_to(info[8 + k : 9 + k], (128, 128)), gate)
        place = dot(named.astype(BF), earlier)
        place = jnp.where(named > 0.5, place + 1.0, 0.0).astype(BF)
        gate_hi = gate.astype(BF)
        gate_lo = (gate - gate_hi.astype(F32)).astype(BF)
        j = slot >> 4
        jc, jh, jl = j >> 4, (j >> 2) & 3, j & 3
        if a == 0:
            ex, ey, ez = x, jl, jh
        elif a == 1:
            ex, ey, ez = jl, y, jh
        else:
            ex, ey, ez = jh, jl, z
        expert = ((ex * 4 + ez) * 2 + jc) * 4 + ey
        pick = (slot_lane == expert).astype(F32).astype(BF)
        match = (dot(pick, place) == ((slot & 3) + 1).astype(F32)) & ((slot_lane >> 5) == ((slot >> 2) & 3))
        sel[a] = jnp.where(match, 1.0, 0.0).astype(BF)
        wgt[a, 0:128] = jnp.where(match, dot(pick, gate_hi), 0.0).T.astype(BF)
        wgt[a, 128:256] = jnp.where(match, dot(pick, gate_lo), 0.0).T.astype(BF)

    def project(*blocks):
        places = []
        for d, e in blocks:
            zz = lax.rem(z + 4 - d, 4)
            xx = lax.rem(x + 4 - e, 4)
            cols = pl.ds(pl.multiple_of(xx * 256, 256), 256)
            c_send[zz, :, cols] = dot(a_buf[zz], b_buf[:, cols]).astype(BF)
            places.append((d, zz, cols))
        for dy in (1, 3, 0, 2):
            yy = lax.rem(y + dy, 4)
            rows = pl.ds(pl.multiple_of(yy * TOK, TOK), TOK)
            for d, zz, cols in places:
                if d or dy:
                    remote(
                        c_send.at[zz, rows, cols], c_recv.at[y * 4 + z, :, cols], c_send_sem, c_recv_sem, (x, yy, zz, c)
                    ).start()
                else:
                    c_recv[y * 4 + z, :, cols] = c_send[zz, rows, cols]

    def columns_half(e, half):
        piece = b_buf.at[pl.ds(half * 512, 512), b_cols(lax.rem(x + 4 - e, 4), c)]
        wait_bytes(piece, b_recv_sem.at[e - 1, half])
        return piece

    def columns_pass(e, half):
        piece = columns_half(e, half)
        remote(piece, piece, b_send_sem, b_recv_sem.at[1, half], (lax.rem(x + e, 4), y, z, c)).start()

    def columns_in(e):
        block = b_buf.at[:, b_cols(lax.rem(x + 4 - e, 4), c)]
        remote(block, block, b_send_sem, b_sib_sem.at[e], sibling).start()

    def columns_ready(e):
        xx = lax.rem(x + 4 - e, 4)
        wait_bytes(b_buf.at[:, b_cols(xx, 1 - c)], b_sib_sem.at[e])

    def heads_ready(d, pair):
        piece = a_buf.at[lax.rem(z + 4 - d, 4), :, pl.ds(pair * 256, 256)]
        wait_bytes(piece, a_recv_sem.at[d - 1, pair])
        return piece

    def heads_pass(d, pair):
        piece = heads_ready(d, pair)
        to = (x, y, lax.rem(z + d, 4), c)
        remote(piece, piece, a_send_sem, a_recv_sem.at[1, pair], to).start()

    heads_pass(1, 0)
    columns_pass(1, 0)
    columns_pass(3, 1)
    heads_pass(1, 1)
    columns_ready(0)
    project((0, 0))
    heads_pass(3, 2)
    heads_pass(3, 3)
    columns_half(1, 1)
    columns_in(1)
    columns_half(3, 0)
    columns_in(3)
    for pair in (2, 3):
        heads_ready(1, pair)
    for pair in (0, 1):
        heads_ready(3, pair)
    columns_ready(1)
    columns_ready(3)

    def far_columns():
        columns_half(2, 0)
        columns_half(2, 1)
        columns_in(2)

    @pl.when(c == 1)
    def _():
        far_columns()
        pl.semaphore_wait(turn_sem, 1)

    for e in (0, 1, 3):
        project((1, e), (3, e), (0, e)) if e else project((1, e), (3, e))

    @pl.when(c == 0)
    def _():
        pl.semaphore_signal(turn_sem, inc=1, device_id=device(*sibling))

    @pl.when(c == 0)
    def _():
        far_columns()

    for pair in range(4):
        heads_ready(2, pair)
    project((2, 0), (2, 1), (2, 3))
    columns_ready(2)
    project((2, 2), (1, 2), (3, 2), (0, 2))
    wait_bytes(c_recv.at[pl.ds(0, 15)], c_recv_sem)
    for copy in takes[7:]:
        copy.wait()
    square = jnp.zeros((TOK, 256), F32)
    for zz in range(4):
        for xx in range(4):
            col = (xx * 4 + zz) * 256
            value = res_ref[:, col : col + 256].astype(F32)
            for yy in range(4):
                value = value + c_recv[yy * 4 + zz, :, xx * 256 : (xx + 1) * 256].astype(F32)
            hid[:, col : col + 256] = value
            square = square + value * value
    scale = lax.rsqrt(jnp.sum(square, axis=-1, keepdims=True) * (1.0 / MODEL) + 1e-06)

    for i, (a, col, width, _) in enumerate(CHUNKS):
        normed = (hid[:, col : col + width] * scale * gain_ref[:, col : col + width]).astype(BF)
        gath[i][along[a]] = normed
        for d in (1, 3, 2):
            to = line_partner(a, x, y, z, d) + (c,)
            mine = gath[i].at[along[a]]
            remote(mine, mine, g_send_sem.at[i], g_recv_sem.at[i], to).start()

    def exchange(members, sources, targets, send_sem, recv_sem, core):
        def put(i, to):
            a = CHUNKS[i][0]
            remote(
                sources[i].at[plane_index(a, *to)],
                targets[i].at[plane_index(a, *me)],
                send_sem.at[i],
                recv_sem.at[i],
                to,
            ).start()

        def step(k, _):
            for i in members:
                px, py, pz, _c = plane_partner(CHUNKS[i][0], x, y, z, c, k * 2)
                put(i, (px, py, pz, core))
            return 0

        lax.fori_loop(1, 16, step, 0)
        if core == 0:
            for i in members:
                put(i, sibling)
                mine = plane_index(CHUNKS[i][0], *me)
                targets[i][mine] = sources[i][mine]

    for group in range(GROUPS):
        for i in range(n):
            if CHUNKS[i][3] == group:
                wait_bytes(gath[i].at[pl.ds(0, 3)], g_recv_sem.at[i])
        for i, (a, col, width, grp) in enumerate(CHUNKS):
            if grp == group:
                rows = dot(sel[a], gath[i][...].reshape(128, width))
                slot_send[i][...] = rows.astype(BF).reshape(32, 16, width)
        members = [i for i in range(n) if CHUNKS[i][3] == group]
        exchange(members, slot_send, slot_recv, s_send_sem, s_recv_sem, 0)
    for group in range(GROUPS):
        members = [i for i in range(n) if CHUNKS[i][3] == group]
        exchange(members, slot_send, slot_recv, s_send_sem, s_recv_sem, 1)

    for copy in loads:
        copy.wait()

    for group in range(GROUPS):
        members = [i for i in range(n) if CHUNKS[i][3] == group]
        for i in members:
            a, col, width, _ = CHUNKS[i]
            wait_bytes(slot_recv[i].at[pl.ds(0, 31)], s_recv_sem.at[i])
            if a != 1:
                for half in range(2):
                    block = slot_recv[i][half * 16 : half * 16 + 16].reshape(256, width)
                    moved = dot(perm[a // 2], block).astype(BF)
                    slot_recv[i][half * 16 : half * 16 + 16] = moved.reshape(16, 16, width)

        def gather_up(cols, members=members, group=group):
            total = proj[:, cols] if group else jnp.zeros((512, 256), F32)
            for i in members:
                _, col, width, _ = CHUNKS[i]
                total = total + dot(slot_recv[i][...].reshape(512, width), w1[col : col + width, cols])
            return total

        def up(t, _, gather_up=gather_up):
            cols = pl.ds(pl.multiple_of(t * 256, 256), 256)
            proj[:, cols] = gather_up(cols)
            return 0

        def last(t, _, gather_up=gather_up):
            first = pl.multiple_of(t * 256, 256)
            gate = gather_up(pl.ds(first, 256))
            value = gather_up(pl.ds(pl.multiple_of(first + FF, 256), 256))
            act[:, pl.ds(first, 256)] = (gate / (1.0 + jnp.exp(-gate)) * value).astype(BF)
            return 0

        if group < GROUPS - 1:
            lax.fori_loop(0, 6, up, 0)
        else:
            lax.fori_loop(0, 3, last, 0)

    for i in range(2):
        for half in range(2):
            rows = slice(half * 256, half * 256 + 256)
            act_p[i, rows, :] = dot(perm_t[i], act[rows, :]).astype(BF)

    for i, (a, col, width, _) in enumerate(CHUNKS):
        wait_bytes(slot_send[i].at[pl.ds(0, 31)], s_send_sem.at[i])
        for t in range(0, width, 256):
            mine = act[...] if a == 1 else act_p[a // 2]
            rows = dot(mine, w2[:, col + t : col + t + 256]).astype(BF)
            slot_send[i][:, :, t : t + 256] = rows.reshape(32, 16, 256)
        for core in range(2):
            exchange([i], slot_send, ret_recv, y_send_sem, y_recv_sem, core)

    for group in range(GROUPS):
        for i, (a, col, width, grp) in enumerate(CHUNKS):
            if grp == group:
                wait_bytes(ret_recv[i].at[pl.ds(0, 31)], y_recv_sem.at[i])
                rows = ret_recv[i][...].reshape(512, width)
                both = dot(wgt[a], rows)
                total = both[0:128] + both[128:256]
                part[i][...] = total.astype(BF).reshape(4, TOK, width)
                part_recv[i][along[a]] = part[i][along[a]]
                for d in (1, 3, 2):
                    to = line_partner(a, x, y, z, d) + (c,)
                    remote(
                        part[i].at[lax.rem(along[a] + d, 4)],
                        part_recv[i].at[along[a]],
                        z_send_sem.at[i],
                        z_recv_sem.at[i],
                        to,
                    ).start()
    for i, (a, col, width, _) in enumerate(CHUNKS):
        wait_bytes(part_recv[i].at[pl.ds(0, 3)], z_recv_sem.at[i])
        total = hid[:, col : col + width]
        for s in range(4):
            total = total + part_recv[i][s].astype(F32)
        out_ref[:, col : col + width] = total.astype(BF)

    wait_bytes(b_buf.at[:, pl.ds(0, 896)], b_send_sem)
    wait_bytes(a_buf.at[pl.ds(0, 3)], a_send_sem)
    wait_bytes(c_recv.at[pl.ds(0, 15)], c_send_sem)
    wait_bytes(meta_all9(meta_all), m_send_sem)
    for i in range(n):
        wait_bytes(gath[i].at[pl.ds(0, 3)], g_send_sem.at[i])
        wait_bytes(slot_send[i].at[pl.ds(0, 31)], y_send_sem.at[i])
        wait_bytes(part[i].at[pl.ds(0, 3)], z_send_sem.at[i])


def meta_all9(meta_all):
    return meta_all.at[:, pl.ds(0, 3)]


def on_device(
    queries, keys, values, document_index, out_proj, residual_in, norm_gain, expert_ids, gate_weights, w_gate_up, w_down
):
    vmem = pl.BlockSpec(memory_space=pltpu.VMEM)
    hbm = pl.BlockSpec(memory_space=pl.ANY)
    dma = pltpu.SemaphoreType.DMA
    n = len(CHUNKS)

    def buf(*shape, dtype=BF):
        return pltpu.VMEM(shape, dtype)

    widths = [chunk[2] for chunk in CHUNKS]
    operands = (
        queries, keys, values, document_index, expert_ids.T, gate_weights.T, out_proj, norm_gain.reshape(1, -1), residual_in
    )
    scratch = [pltpu.VMEM(value.shape, value.dtype) for value in operands]
    scratch += [
        buf(MODEL, 2 * FF),
        buf(FF, MODEL),
        buf(1024, 1024),
        buf(4, 128, 1024),
        buf(4, 128, 1024),
        buf(16, TOK, 1024),
        buf(TOK, MODEL, dtype=F32),
        buf(512, 2 * FF, dtype=F32),
        buf(512, FF),
        buf(2, 512, FF),
        buf(16, 128, dtype=F32),
        buf(8, 128, dtype=F32),
        buf(3, 4, 16, 128, dtype=F32),
        buf(3, 512, 128),
        buf(3, 256, 512),
        buf(2, 256, 256),
        buf(2, 256, 256),
    ]
    scratch += [buf(4, TOK, w) for w in widths]
    for _ in range(3):
        scratch += [buf(32, 16, w) for w in widths]
    for _ in range(2):
        scratch += [buf(4, TOK, w) for w in widths]
    scratch += [
        pltpu.SemaphoreType.REGULAR, dma((9,)), dma((6,)), dma, dma((3, 2)), dma((4,)), dma, dma((3, 4)), dma, dma, dma, dma,
        dma((n,)), dma((n,)), dma((n,)), dma((n,)), dma((n,)), dma((n,)), dma((n,)), dma((n,)),
    ]
    out = pl.pallas_call(
        kernel,
        out_shape=pltpu.VMEM((TOK, MODEL), BF),
        in_specs=[hbm] * 11,
        out_specs=vmem,
        scratch_shapes=scratch,
        name="layer",
        compiler_params=pltpu.CompilerParams(
            collective_id=0, has_side_effects=True, vmem_limit_bytes=60_000_000
        ),
    )(*operands, w_gate_up, w_down)
    return out


def solution(mesh):
    both = P(("group", "tensor"), None)
    expert = P(("group", "tensor"), None, None)
    pair = P("group", "tensor")
    in_specs = (pair, pair, pair, P("group", None), P("tensor", "group"), both, P(), both, both, expert, expert)
    return jax.shard_map(on_device, mesh=mesh, in_specs=in_specs, out_specs=both, check_vma=False)
```

```python
import functools

import jax
import jax.numpy as jnp
from jax import lax
from jax.experimental import pallas as pl
from jax.experimental.pallas import tpu as pltpu
from jax.sharding import PartitionSpec as P

HEAD = 128
MODEL = 4096
FF = 768
TOK = 32
CHUNKS = (
    (1, 1280, 512, 0),
    (0, 0, 512, 0),
    (2, 2560, 512, 0),
    (1, 1792, 512, 1),
    (0, 512, 512, 1),
    (2, 3072, 512, 1),
    (1, 2304, 256, 2),
    (0, 1024, 256, 2),
    (2, 3584, 512, 2),
)
GROUPS = 3
BF = jnp.bfloat16
F32 = jnp.float32


def dot(a, b):
    return jnp.dot(a, b, preferred_element_type=F32)


def device(x, y, z, c):
    return {"group": (x * 4 + z) * 2 + c, "tensor": y}


def plane_index(a, x, y, z, c):
    if a == 0:
        return c * 16 + z * 4 + y
    if a == 1:
        return c * 16 + z * 4 + x
    return c * 16 + x * 4 + y


def plane_partner(a, x, y, z, c, k):
    nc = lax.rem(c + lax.rem(k, 2), 2)
    lo = lax.rem(k // 2, 4)
    hi = k // 8
    if a == 0:
        return x, lax.rem(y + lo, 4), lax.rem(z + hi, 4), nc
    if a == 1:
        return lax.rem(x + lo, 4), y, lax.rem(z + hi, 4), nc
    return lax.rem(x + hi, 4), lax.rem(y + lo, 4), z, nc


def line_partner(a, x, y, z, d):
    if a == 0:
        return lax.rem(x + d, 4), y, z
    if a == 1:
        return x, lax.rem(y + d, 4), z
    return x, y, lax.rem(z + d, 4)


def axis_row(a, canon):
    r = canon & 3
    y = (canon >> 2) & 3
    x = (canon >> 4) & 3
    z = (canon >> 6) & 3
    if a == 0:
        return z * 64 + y * 16 + x * 4 + r
    return x * 64 + y * 16 + z * 4 + r


def iota(shape, dim):
    return lax.broadcasted_iota(jnp.int32, shape, dim)


def kernel(
    *refs
):
    n = len(CHUNKS)
    operands, (w1_hbm, w2_hbm, out_ref), inputs, scratch = refs[:9], refs[9:12], refs[12:21], refs[21:]
    q_ref, k_ref, v_ref, doc_ref, ids_ref, gates_ref, wo_ref, gain_ref, res_ref = inputs
    (w1, w2, b_buf, a_buf, c_send, c_recv, hid, proj, act, act_p, meta, turn, meta_all, sel, wgt, perm, perm_t) = scratch[:17]
    rest = scratch[17:]
    gath, slot_send, slot_recv, ret_recv, part, part_recv = (rest[i * n : (i + 1) * n] for i in range(6))
    (
        turn_sem, in_sem, w_sem, b_send_sem, b_recv_sem, b_sib_sem, a_send_sem, a_recv_sem, c_send_sem, c_recv_sem, m_send_sem, m_recv_sem,
        g_send_sem, g_recv_sem, s_send_sem, s_recv_sem, y_send_sem, y_recv_sem, z_send_sem, z_recv_sem,
    ) = rest[6 * n :]

    g = lax.axis_index("group")
    y = lax.axis_index("tensor")
    x = g // 8
    z = lax.rem(g // 2, 4)
    c = lax.rem(g, 2)
    me = (x, y, z, c)
    along = (x, y, z)

    def remote(src, dst, send, recv, to):
        return pltpu.make_async_remote_copy(
            src_ref=src, dst_ref=dst, send_sem=send, recv_sem=recv, device_id=device(*to)
        )

    def wait_bytes(ref, sem):
        pltpu.make_async_copy(ref, ref, sem).wait()

    takes = [pltpu.make_async_copy(src, dst, in_sem.at[i]) for i, (src, dst) in enumerate(zip(operands, inputs))]
    for copy in takes:
        copy.start()
    barrier = pltpu.get_barrier_semaphore()

    def greet(to):
        pl.semaphore_signal(barrier, inc=1, device_id=device(*to))
        return 0

    lax.fori_loop(1, 4, lambda k, _: greet((lax.rem(x + k, 4), y, z, c)), 0)
    greet((x, y, z, 1 - c))
    lax.fori_loop(1, 16, lambda k, _: greet((x, lax.rem(y + k // 4, 4), lax.rem(z + k, 4), c)), 0)

    for copy in takes[:6]:
        copy.wait()
    doc = jnp.broadcast_to(doc_ref[...].astype(F32), (128, 128))
    visible = (doc == doc.T) & (iota((128, 128), 0) >= iota((128, 128), 1))
    keys = k_ref[...]
    vals = v_ref[...]

    def attend(h):
        query = q_ref[:, h * HEAD : (h + 1) * HEAD]
        scores = lax.dot_general(query, keys, (((1,), (1,)), ((), ())), preferred_element_type=F32)
        scores = jnp.where(visible, scores * (1.0 / HEAD**0.5), -1e30)
        top = jnp.max(scores, axis=-1, keepdims=True)
        expo = jnp.where(visible, jnp.exp(scores - top), 0.0)
        weights = (expo / jnp.sum(expo, axis=-1, keepdims=True)).astype(BF)
        a_buf[z, :, h * HEAD : (h + 1) * HEAD] = dot(weights, vals).astype(BF)

    def send_heads(d, pair):
        cols = pl.ds(pair * 256, 256)
        to = (x, y, lax.rem(z + d, 4), c)
        remote(a_buf.at[z, :, cols], a_buf.at[z, :, cols], a_send_sem, a_recv_sem.at[d - 1, pair], to).start()

    def b_cols(xx, cc):
        return pl.ds(pl.multiple_of((xx * 2 + cc) * 128, 128), 128)

    lanes = iota((8, 128), 1)
    for i, ref in enumerate((ids_ref, gates_ref)):
        turn[:, 0:TOK] = ref[...].astype(F32)
        once = jnp.where(lanes < TOK, turn[...], 0.0)
        meta[8 * i : 8 * i + 8] = once + sum(pltpu.roll(once, TOK * s, 1) for s in (1, 2, 3))
    for h in range(2):
        attend(h)
    takes[6].wait()
    pl.semaphore_wait(barrier, 19)
    sibling = (x, y, z, 1 - c)
    for a in range(3):
        for d in (1, 3, 2):
            to = line_partner(a, x, y, z, d) + (c,)
            remote(meta, meta_all.at[a, along[a]], m_send_sem, m_recv_sem, to).start()
    remote(wo_ref, b_buf.at[:, b_cols(x, c)], b_send_sem, b_sib_sem.at[0], sibling).start()
    for d, halves in ((1, (0, 1)), (3, (1, 0))):
        for half in halves:
            rows = pl.ds(half * 512, 512)
            to = (lax.rem(x + d, 4), y, z, c)
            remote(
                wo_ref.at[rows, :], b_buf.at[rows, b_cols(x, c)], b_send_sem, b_recv_sem.at[d - 1, half], to
            ).start()

    @pl.when(c == 0)
    def _():
        send_heads(1, 0)
        send_heads(3, 0)

    loads = []
    for i in range(4):
        loads.append(
            pltpu.make_async_copy(w1_hbm.at[0, pl.ds(i * 1024, 1024)], w1.at[pl.ds(i * 1024, 1024)], w_sem.at[i])
        )
    for i in range(2):
        loads.append(
            pltpu.make_async_copy(w2_hbm.at[0, pl.ds(i * 384, 384)], w2.at[pl.ds(i * 384, 384)], w_sem.at[4 + i])
        )
    for copy in loads:
        copy.start()

    for pair in range(1, 4):
        for h in (2 * pair, 2 * pair + 1):
            attend(h)

        @pl.when(c == 0)
        def _(pair=pair):
            send_heads(1, pair)
            if pair > 1:
                send_heads(3, pair)

    @pl.when(c == 0)
    def _():
        send_heads(3, 1)

    @pl.when(c == 1)
    def _():
        for up, down in ((0, 2), (1, 3), (2, 0), (3, 1)):
            send_heads(1, up)
            send_heads(3, down)

    b_buf[:, b_cols(x, c)] = wo_ref[...]

    for a in range(3):
        meta_all[a, along[a]] = meta[...]
    canon = iota((256, 256), 0)
    canon_t = iota((256, 256), 1)
    for i, a in enumerate((0, 2)):
        perm[i] = (iota((256, 256), 1) == axis_row(a, canon)).astype(F32).astype(BF)
        perm_t[i] = (iota((256, 256), 0) == axis_row(a, canon_t)).astype(F32).astype(BF)
    wait_bytes(meta_all9(meta_all), m_recv_sem)
    lane = iota((128, 128), 1)
    row = iota((128, 128), 0)
    earlier = (((row >> 5) == (lane >> 5)) & (row < lane)).astype(F32).astype(BF)
    slot = iota((512, 128), 0)
    slot_lane = iota((512, 128), 1)
    for a in range(3):
        info = jnp.zeros((16, 128), F32)
        for s in range(4):
            info = jnp.where((iota((16, 128), 1) >> 5) == s, meta_all[a, s], info)
        named = jnp.zeros((128, 128), F32)
        gate = jnp.zeros((128, 128), F32)
        row_f = row.astype(F32)
        for k in range(8):
            hit = jnp.broadcast_to(info[k : k + 1], (128, 128)) == row_f
            named = jnp.where(hit, 1.0, named)
            gate = jnp.where(hit, jnp.broadcast_to(info[8 + k : 9 + k], (128, 128)), gate)
        place = dot(named.astype(BF), earlier)
        place = jnp.where(named > 0.5, place + 1.0, 0.0).astype(BF)
        gate_hi = gate.astype(BF)
        gate_lo = (gate - gate_hi.astype(F32)).astype(BF)
        j = slot >> 4
        jc, jh, jl = j >> 4, (j >> 2) & 3, j & 3
        if a == 0:
            ex, ey, ez = x, jl, jh
        elif a == 1:
            ex, ey, ez = jl, y, jh
        else:
            ex, ey, ez = jh, jl, z
        expert = ((ex * 4 + ez) * 2 + jc) * 4 + ey
        pick = (slot_lane == expert).astype(F32).astype(BF)
        match = (dot(pick, place) == ((slot & 3) + 1).astype(F32)) & ((slot_lane >> 5) == ((slot >> 2) & 3))
        sel[a] = jnp.where(match, 1.0, 0.0).astype(BF)
        wgt[a, 0:128] = jnp.where(match, dot(pick, gate_hi), 0.0).T.astype(BF)
        wgt[a, 128:256] = jnp.where(match, dot(pick, gate_lo), 0.0).T.astype(BF)

    def project(*blocks):
        places = []
        for d, e in blocks:
            zz = lax.rem(z + 4 - d, 4)
            xx = lax.rem(x + 4 - e, 4)
            cols = pl.ds(pl.multiple_of(xx * 256, 256), 256)
            c_send[zz, :, cols] = dot(a_buf[zz], b_buf[:, cols]).astype(BF)
            places.append((d, zz, cols))
        for dy in (1, 3, 0, 2):
            yy = lax.rem(y + dy, 4)
            rows = pl.ds(pl.multiple_of(yy * TOK, TOK), TOK)
            for d, zz, cols in places:
                if d or dy:
                    remote(
                        c_send.at[zz, rows, cols], c_recv.at[y * 4 + z, :, cols], c_send_sem, c_recv_sem, (x, yy, zz, c)
                    ).start()
                else:
                    c_recv[y * 4 + z, :, cols] = c_send[zz, rows, cols]

    def columns_half(e, half):
        piece = b_buf.at[pl.ds(half * 512, 512), b_cols(lax.rem(x + 4 - e, 4), c)]
        wait_bytes(piece, b_recv_sem.at[e - 1, half])
        return piece

    def columns_pass(e, half):
        piece = columns_half(e, half)
        remote(piece, piece, b_send_sem, b_recv_sem.at[1, half], (lax.rem(x + e, 4), y, z, c)).start()

    def columns_in(e):
        block = b_buf.at[:, b_cols(lax.rem(x + 4 - e, 4), c)]
        remote(block, block, b_send_sem, b_sib_sem.at[e], sibling).start()

    def columns_ready(e):
        xx = lax.rem(x + 4 - e, 4)
        wait_bytes(b_buf.at[:, b_cols(xx, 1 - c)], b_sib_sem.at[e])

    def heads_ready(d, pair):
        piece = a_buf.at[lax.rem(z + 4 - d, 4), :, pl.ds(pair * 256, 256)]
        wait_bytes(piece, a_recv_sem.at[d - 1, pair])
        return piece

    def heads_pass(d, pair):
        piece = heads_ready(d, pair)
        to = (x, y, lax.rem(z + d, 4), c)
        remote(piece, piece, a_send_sem, a_recv_sem.at[1, pair], to).start()

    heads_pass(1, 0)
    columns_pass(1, 0)
    columns_pass(3, 1)
    heads_pass(1, 1)
    columns_ready(0)
    project((0, 0))
    heads_pass(3, 2)
    heads_pass(3, 3)
    columns_half(1, 1)
    columns_in(1)
    columns_half(3, 0)
    columns_in(3)
    for pair in (2, 3):
        heads_ready(1, pair)
    for pair in (0, 1):
        heads_ready(3, pair)
    columns_ready(1)
    columns_ready(3)

    def far_columns():
        columns_half(2, 0)
        columns_half(2, 1)
        columns_in(2)

    @pl.when(c == 1)
    def _():
        far_columns()
        pl.semaphore_wait(turn_sem, 1)

    for e in (0, 1, 3):
        project((1, e), (3, e), (0, e)) if e else project((1, e), (3, e))

    @pl.when(c == 0)
    def _():
        pl.semaphore_signal(turn_sem, inc=1, device_id=device(*sibling))

    @pl.when(c == 0)
    def _():
        far_columns()

    for pair in range(4):
        heads_ready(2, pair)
    project((2, 0), (2, 1), (2, 3))
    columns_ready(2)
    project((2, 2), (1, 2), (3, 2), (0, 2))
    wait_bytes(c_recv.at[pl.ds(0, 15)], c_recv_sem)
    for copy in takes[7:]:
        copy.wait()
    square = jnp.zeros((TOK, 256), F32)
    for zz in range(4):
        for xx in range(4):
            col = (xx * 4 + zz) * 256
            value = res_ref[:, col : col + 256].astype(F32)
            for yy in range(4):
                value = value + c_recv[yy * 4 + zz, :, xx * 256 : (xx + 1) * 256].astype(F32)
            hid[:, col : col + 256] = value
            square = square + value * value
    scale = lax.rsqrt(jnp.sum(square, axis=-1, keepdims=True) * (1.0 / MODEL) + 1e-06)

    for i, (a, col, width, _) in enumerate(CHUNKS):
        normed = (hid[:, col : col + width] * scale * gain_ref[:, col : col + width]).astype(BF)
        gath[i][along[a]] = normed
        for d in (1, 3, 2):
            to = line_partner(a, x, y, z, d) + (c,)
            mine = gath[i].at[along[a]]
            remote(mine, mine, g_send_sem.at[i], g_recv_sem.at[i], to).start()

    def exchange(members, sources, targets, send_sem, recv_sem, core):
        def put(i, to):
            a = CHUNKS[i][0]
            remote(
                sources[i].at[plane_index(a, *to)],
                targets[i].at[plane_index(a, *me)],
                send_sem.at[i],
                recv_sem.at[i],
                to,
            ).start()

        def step(k, _):
            for i in members:
                px, py, pz, _c = plane_partner(CHUNKS[i][0], x, y, z, c, lax.rem(k * 5, 16) * 2)
                put(i, (px, py, pz, core))
            return 0

        lax.fori_loop(1, 16, step, 0)
        if core == 0:
            for i in members:
                put(i, sibling)
                mine = plane_index(CHUNKS[i][0], *me)
                targets[i][mine] = sources[i][mine]

    for group in range(GROUPS):
        for i in range(n):
            if CHUNKS[i][3] == group:
                wait_bytes(gath[i].at[pl.ds(0, 3)], g_recv_sem.at[i])
        for i, (a, col, width, grp) in enumerate(CHUNKS):
            if grp == group:
                rows = dot(sel[a], gath[i][...].reshape(128, width))
                slot_send[i][...] = rows.astype(BF).reshape(32, 16, width)
        members = [i for i in range(n) if CHUNKS[i][3] == group]
        exchange(members, slot_send, slot_recv, s_send_sem, s_recv_sem, 0)
    for group in range(GROUPS):
        members = [i for i in range(n) if CHUNKS[i][3] == group]
        exchange(members, slot_send, slot_recv, s_send_sem, s_recv_sem, 1)

    for copy in loads:
        copy.wait()

    for group in range(GROUPS):
        members = [i for i in range(n) if CHUNKS[i][3] == group]
        for i in members:
            a, col, width, _ = CHUNKS[i]
            wait_bytes(slot_recv[i].at[pl.ds(0, 31)], s_recv_sem.at[i])
            if a != 1:
                for half in range(2):
                    block = slot_recv[i][half * 16 : half * 16 + 16].reshape(256, width)
                    moved = dot(perm[a // 2], block).astype(BF)
                    slot_recv[i][half * 16 : half * 16 + 16] = moved.reshape(16, 16, width)

        def gather_up(cols, members=members, group=group):
            total = proj[:, cols] if group else jnp.zeros((512, 256), F32)
            for i in members:
                _, col, width, _ = CHUNKS[i]
                total = total + dot(slot_recv[i][...].reshape(512, width), w1[col : col + width, cols])
            return total

        def up(t, _, gather_up=gather_up):
            cols = pl.ds(pl.multiple_of(t * 256, 256), 256)
            proj[:, cols] = gather_up(cols)
            return 0

        def last(t, _, gather_up=gather_up):
            first = pl.multiple_of(t * 256, 256)
            gate = gather_up(pl.ds(first, 256))
            value = gather_up(pl.ds(pl.multiple_of(first + FF, 256), 256))
            act[:, pl.ds(first, 256)] = (gate / (1.0 + jnp.exp(-gate)) * value).astype(BF)
            return 0

        if group < GROUPS - 1:
            lax.fori_loop(0, 6, up, 0)
        else:
            lax.fori_loop(0, 3, last, 0)

    for i in range(2):
        for half in range(2):
            rows = slice(half * 256, half * 256 + 256)
            act_p[i, rows, :] = dot(perm_t[i], act[rows, :]).astype(BF)

    for group in range(GROUPS):
        for i, (a, col, width, grp) in enumerate(CHUNKS):
            if grp == group:
                wait_bytes(slot_send[i].at[pl.ds(0, 31)], s_send_sem.at[i])
                for t in range(0, width, 256):
                    mine = act[...] if a == 1 else act_p[a // 2]
                    rows = dot(mine, w2[:, col + t : col + t + 256]).astype(BF)
                    slot_send[i][:, :, t : t + 256] = rows.reshape(32, 16, 256)
        members = [i for i in range(n) if CHUNKS[i][3] == group]
        for core in range(2):
            exchange(members, slot_send, ret_recv, y_send_sem, y_recv_sem, core)

    for group in range(GROUPS):
        for i, (a, col, width, grp) in enumerate(CHUNKS):
            if grp == group:
                wait_bytes(ret_recv[i].at[pl.ds(0, 31)], y_recv_sem.at[i])
                rows = ret_recv[i][...].reshape(512, width)
                both = dot(wgt[a], rows)
                total = both[0:128] + both[128:256]
                part[i][...] = total.astype(BF).reshape(4, TOK, width)
                part_recv[i][along[a]] = part[i][along[a]]
                for d in (1, 3, 2):
                    to = line_partner(a, x, y, z, d) + (c,)
                    remote(
                        part[i].at[lax.rem(along[a] + d, 4)],
                        part_recv[i].at[along[a]],
                        z_send_sem.at[i],
                        z_recv_sem.at[i],
                        to,
                    ).start()
    for i, (a, col, width, _) in enumerate(CHUNKS):
        wait_bytes(part_recv[i].at[pl.ds(0, 3)], z_recv_sem.at[i])
        total = hid[:, col : col + width]
        for s in range(4):
            total = total + part_recv[i][s].astype(F32)
        out_ref[:, col : col + width] = total.astype(BF)

    wait_bytes(b_buf.at[:, pl.ds(0, 896)], b_send_sem)
    wait_bytes(a_buf.at[pl.ds(0, 3)], a_send_sem)
    wait_bytes(c_recv.at[pl.ds(0, 15)], c_send_sem)
    wait_bytes(meta_all9(meta_all), m_send_sem)
    for i in range(n):
        wait_bytes(gath[i].at[pl.ds(0, 3)], g_send_sem.at[i])
        wait_bytes(slot_send[i].at[pl.ds(0, 31)], y_send_sem.at[i])
        wait_bytes(part[i].at[pl.ds(0, 3)], z_send_sem.at[i])


def meta_all9(meta_all):
    return meta_all.at[:, pl.ds(0, 3)]


def on_device(
    queries, keys, values, document_index, out_proj, residual_in, norm_gain, expert_ids, gate_weights, w_gate_up, w_down
):
    vmem = pl.BlockSpec(memory_space=pltpu.VMEM)
    hbm = pl.BlockSpec(memory_space=pl.ANY)
    dma = pltpu.SemaphoreType.DMA
    n = len(CHUNKS)

    def buf(*shape, dtype=BF):
        return pltpu.VMEM(shape, dtype)

    widths = [chunk[2] for chunk in CHUNKS]
    operands = (
        queries, keys, values, document_index, expert_ids.T, gate_weights.T, out_proj, norm_gain.reshape(1, -1), residual_in
    )
    scratch = [pltpu.VMEM(value.shape, value.dtype) for value in operands]
    scratch += [
        buf(MODEL, 2 * FF),
        buf(FF, MODEL),
        buf(1024, 1024),
        buf(4, 128, 1024),
        buf(4, 128, 1024),
        buf(16, TOK, 1024),
        buf(TOK, MODEL, dtype=F32),
        buf(512, 2 * FF, dtype=F32),
        buf(512, FF),
        buf(2, 512, FF),
        buf(16, 128, dtype=F32),
        buf(8, 128, dtype=F32),
        buf(3, 4, 16, 128, dtype=F32),
        buf(3, 512, 128),
        buf(3, 256, 512),
        buf(2, 256, 256),
        buf(2, 256, 256),
    ]
    scratch += [buf(4, TOK, w) for w in widths]
    for _ in range(3):
        scratch += [buf(32, 16, w) for w in widths]
    for _ in range(2):
        scratch += [buf(4, TOK, w) for w in widths]
    scratch += [
        pltpu.SemaphoreType.REGULAR, dma((9,)), dma((6,)), dma, dma((3, 2)), dma((4,)), dma, dma((3, 4)), dma, dma, dma, dma,
        dma((n,)), dma((n,)), dma((n,)), dma((n,)), dma((n,)), dma((n,)), dma((n,)), dma((n,)),
    ]
    out = pl.pallas_call(
        kernel,
        out_shape=pltpu.VMEM((TOK, MODEL), BF),
        in_specs=[hbm] * 11,
        out_specs=vmem,
        scratch_shapes=scratch,
        name="layer",
        compiler_params=pltpu.CompilerParams(
            collective_id=0, has_side_effects=True, vmem_limit_bytes=60_000_000
        ),
    )(*operands, w_gate_up, w_down)
    return out


def solution(mesh):
    both = P(("group", "tensor"), None)
    expert = P(("group", "tensor"), None, None)
    pair = P("group", "tensor")
    in_specs = (pair, pair, pair, P("group", None), P("tensor", "group"), both, P(), both, both, expert, expert)
    return jax.shard_map(on_device, mesh=mesh, in_specs=in_specs, out_specs=both, check_vma=False)
```
